8 devices in a mesh: tp: 4 (over z, y, x), dp: 2 (over core).
Axes of the slice: x: 2, y: 2, z: 1, core: 2. Of those that a mesh axis runs over, the one named last changes fastest.
Arguments:
- x: bfloat16 [6144, 5120], P(('dp', 'tp'))
- w_gate: bfloat16 [5120, 13824], P('dp', 'tp')
- w_up: bfloat16 [5120, 13824], P('dp', 'tp')
- w_down: bfloat16 [13824, 5120], P('tp', 'dp')
- dy: bfloat16 [6144, 5120], P(('dp', 'tp'))
Outputs:
- output 1: bfloat16 [6144, 5120], P(('dp', 'tp'))
- output 2: bfloat16 [6144, 5120], P(('dp', 'tp'))
- output 3: float32 [5120, 13824], P('dp', 'tp')
- output 4: float32 [5120, 13824], P('dp', 'tp')
- output 5: float32 [13824, 5120], P('tp', 'dp')
All inputs are finite; a program needn't handle non-finite values.
Results may differ from the reference program's by a relative error of at most 0.00119.
Values are sent between devices in bfloat16 or wider.
A program may use at most 1 GiB of HBM per device.

```python
import jax
import jax.numpy as jnp
from jax import lax

ROWS = 6144
D = 5120
FF = 13824


def setup_inputs(seed: int = 0) -> dict:
    ks = jax.random.split(jax.random.key(seed), 5)
    x = jax.random.normal(ks[0], (ROWS, D), jnp.float32)
    w_gate = jax.random.normal(ks[1], (D, FF), jnp.float32) * (D ** -0.5)
    w_up = jax.random.normal(ks[2], (D, FF), jnp.float32) * (D ** -0.5)
    w_down = jax.random.normal(ks[3], (FF, D), jnp.float32) * (1.5 * FF ** -0.5)
    dy = jax.random.normal(ks[4], (ROWS, D), jnp.float32)
    return dict(x=x.astype(jnp.bfloat16), w_gate=w_gate.astype(jnp.bfloat16), w_up=w_up.astype(jnp.bfloat16), w_down=w_down.astype(jnp.bfloat16), dy=dy.astype(jnp.bfloat16))


def reference(x, w_gate, w_up, w_down, dy):
    nb = ROWS // 256
    xs = x.reshape(nb, ROWS // nb, D)
    dys = dy.reshape(nb, ROWS // nb, D)

    def body(carry, inp):
        gw, uw, dw = carry
        xb, dyb = inp
        a = jnp.dot(xb, w_gate, preferred_element_type=jnp.float32)
        b = jnp.dot(xb, w_up, preferred_element_type=jnp.float32)
        sig = jax.nn.sigmoid(a)
        sa = a * sig
        h = (sa * b).astype(jnp.bfloat16)
        y = (xb.astype(jnp.float32) + jnp.dot(h, w_down, preferred_element_type=jnp.float32)).astype(jnp.bfloat16)
        g = jnp.dot(dyb, w_down.T, preferred_element_type=jnp.float32)
        da = (g * b * sig * (1.0 + a * (1.0 - sig))).astype(jnp.bfloat16)
        db = (g * sa).astype(jnp.bfloat16)
        dx = (dyb.astype(jnp.float32) + jnp.dot(da, w_gate.T, preferred_element_type=jnp.float32) + jnp.dot(db, w_up.T, preferred_element_type=jnp.float32)).astype(jnp.bfloat16)
        gw = gw + jnp.dot(xb.T, da, preferred_element_type=jnp.float32)
        uw = uw + jnp.dot(xb.T, db, preferred_element_type=jnp.float32)
        dw = dw + jnp.dot(h.T, dyb, preferred_element_type=jnp.float32)
        return (gw, uw, dw), (y, dx)

    init = (jnp.zeros((D, FF), jnp.float32), jnp.zeros((D, FF), jnp.float32), jnp.zeros((FF, D), jnp.float32))
    (gw, uw, dw), (ys, dxs) = lax.scan(body, init, (xs, dys))
    return ys.reshape(ROWS, D), dxs.reshape(ROWS, D), gw, uw, dw
```

```python
import jax
import jax.numpy as jnp
from jax import lax
from jax.experimental import pallas as pl
from jax.experimental.pallas import tpu as pltpu
from jax.sharding import PartitionSpec as P


f32 = jnp.float32
bf = jnp.bfloat16
NT = (((1,), (1,)), ((), ()))
TN = (((0,), (0,)), ((), ()))
VMEM = 62 * 1024 * 1024
ONE = pl.Buffered(1)
ANY = pl.BlockSpec(memory_space=pl.ANY)


def mm(u, v):
    return jnp.dot(u, v, preferred_element_type=f32)


def dg(u, v, dims):
    return lax.dot_general(u, v, dims, preferred_element_type=f32)


def sds(shape, dtype):
    return jax.ShapeDtypeStruct(shape, dtype)


def spec(shape, index, once=False):
    if once:
        return pl.BlockSpec(shape, index, pipeline_mode=ONE)
    return pl.BlockSpec(shape, index)


def row_loop(rows, step, fn):
    def trip(m, carry):
        fn(pl.ds(pl.multiple_of(m * step, step), step))
        return carry

    lax.fori_loop(0, rows // step, trip, 0)


def call(body, core, grid, ins, outs, args, flops, scratch=(), aliases=None):
    moved = sum(a.size * a.dtype.itemsize for a in args)
    return pl.pallas_call(
        body,
        grid_spec=pltpu.PrefetchScalarGridSpec(
            num_scalar_prefetch=1, grid=grid, in_specs=list(ins), out_specs=[o[0] for o in outs], scratch_shapes=list(scratch)
        ),
        out_shape=[sds(o[1], o[2]) for o in outs],
        input_output_aliases=aliases or {},
        compiler_params=pltpu.CompilerParams(dimension_semantics=("arbitrary",) * len(grid), vmem_limit_bytes=VMEM),
        cost_estimate=pl.CostEstimate(flops=int(flops), bytes_accessed=int(moved), transcendentals=0),
    )(core, *args)


def silu_h(a, b):
    return (a * jax.nn.sigmoid(a) * b).astype(bf)


def k_fwd0(core, x, wg, wgo, wu, wuo, tn=512):
    r, d = x.shape
    hd, f = wg.shape
    steps = pl.cdiv(f, tn)
    last = f - (steps - 1) * tn

    def body(i_ref, x_ref, wg_ref, wgo_ref, wu_ref, wuo_ref, a_ref, b_ref, h_ref, hall_ref, xall_ref, wgc_ref, wuc_ref, sem, wsem):
        n = pl.program_id(0)
        s = pl.multiple_of(i_ref[0] * hd, 128)
        o = pl.multiple_of((1 - i_ref[0]) * hd, 128)
        keep_x = pltpu.make_async_copy(x_ref, xall_ref.at[pl.ds(0, r), :], sem)

        def copies(width):
            c = pl.ds(pl.multiple_of(n * tn, 128), width)
            moves = ((wg_ref, wgc_ref, s), (wgo_ref, wgc_ref, o), (wu_ref, wuc_ref, s), (wuo_ref, wuc_ref, o))
            return [
                pltpu.make_async_copy(u.at[:, pl.ds(0, width)], v.at[pl.ds(q, hd), c], wsem.at[k])
                for k, (u, v, q) in enumerate(moves)
            ]

        @pl.when(n == 0)
        def _():
            keep_x.start()

        @pl.when(n < steps - 1)
        def _():
            for c in copies(tn):
                c.start()

        @pl.when(n == steps - 1)
        def _():
            for c in copies(last):
                c.start()

        def rows(m):
            xs = x_ref[m, pl.ds(s, hd)]
            xo = x_ref[m, pl.ds(o, hd)]
            a = mm(xs, wg_ref[...]) + mm(xo, wgo_ref[...])
            b = mm(xs, wu_ref[...]) + mm(xo, wuo_ref[...])
            a_ref[m, :] = a
            b_ref[m, :] = b
            h = silu_h(a, b)
            h_ref[m, :] = h
            hall_ref[m, :] = h

        row_loop(r, 256, rows)

        @pl.when(n < steps - 1)
        def _():
            for c in copies(tn):
                c.wait()

        @pl.when(n == steps - 1)
        def _():
            for c in copies(last):
                c.wait()
            keep_x.wait()

    w = spec((hd, tn), lambda n, i: (0, n))
    o = spec((r, tn), lambda n, i: (0, n))
    return call(
        body, core, (steps,),
        [spec((r, d), lambda n, i: (0, 0), True), w, w, w, w],
        [(o, (r, f), f32), (o, (r, f), f32), (o, (r, f), bf), (o, (4 * r, f), bf), (ANY, (4 * r, d), bf),
         (ANY, (d, f), bf), (ANY, (d, f), bf)],
        (x, wg, wgo, wu, wuo), 4 * r * d * f,
        scratch=[pltpu.SemaphoreType.DMA, pltpu.SemaphoreType.DMA((4,))],
    )


def k_fwd(core, slot, x, wg, wu, hall, xall, tn=512):
    r, d = x.shape
    f = wg.shape[1]
    steps = pl.cdiv(f, tn)

    def body(i_ref, x_ref, wg_ref, wu_ref, hin_ref, xin_ref, a_ref, b_ref, h_ref, hall_ref, xall_ref, sem):
        n = pl.program_id(0)
        keep_x = pltpu.make_async_copy(x_ref, xall_ref.at[pl.ds(slot * r, r), :], sem)

        @pl.when(n == 0)
        def _():
            keep_x.start()

        def rows(m):
            a = mm(x_ref[m, :], wg_ref[...])
            b = mm(x_ref[m, :], wu_ref[...])
            a_ref[m, :] = a
            b_ref[m, :] = b
            h = silu_h(a, b)
            h_ref[m, :] = h
            hall_ref[m, :] = h

        row_loop(r, 256, rows)

        @pl.when(n == steps - 1)
        def _():
            keep_x.wait()

    w = spec((d, tn), lambda n, i: (0, n))
    o = spec((r, tn), lambda n, i: (0, n))
    return call(
        body, core, (steps,),
        [spec((r, d), lambda n, i: (0, 0), True), w, w, ANY, ANY],
        [(o, (r, f), f32), (o, (r, f), f32), (o, (r, f), bf),
         (spec((r, tn), lambda n, i: (slot, n)), (4 * r, f), bf), (ANY, (4 * r, d), bf)],
        (x, wg, wu, hall, xall), 4 * r * d * f,
        scratch=[pltpu.SemaphoreType.DMA], aliases={4: 3, 5: 4},
    )


def k_y0(core, h, wd, wdo, tn=512):
    r, f = h.shape
    hd = wd.shape[1]
    nt = hd // tn

    def body(i_ref, h_ref, w_ref, wo_ref, o_ref, wc_ref, sem):
        n = pl.program_id(0)
        own = (n < nt) == (i_ref[0] == 0)

        def part(w):
            keep = pltpu.make_async_copy(w, wc_ref.at[:, pl.ds(pl.multiple_of(n * tn, 128), tn)], sem)
            keep.start()

            def rows(m):
                o_ref[m, :] = mm(h_ref[m, :], w[...])

            row_loop(r, 256, rows)
            keep.wait()

        @pl.when(own)
        def _():
            part(w_ref)

        @pl.when(jnp.logical_not(own))
        def _():
            part(wo_ref)

    return call(
        body, core, (2 * nt,),
        [spec((r, f), lambda n, i: (0, 0), True),
         spec((f, tn), lambda n, i: (0, jnp.clip(n - i[0] * nt, 0, nt - 1))),
         spec((f, tn), lambda n, i: (0, jnp.clip(n - (1 - i[0]) * nt, 0, nt - 1)))],
        [(spec((r, tn), lambda n, i: (0, n)), (r, 2 * hd), f32), (ANY, (f, 2 * hd), bf)],
        (h, wd, wdo), 4 * r * hd * f,
        scratch=[pltpu.SemaphoreType.DMA],
    )


def k_y(core, h, wd, add=None, tn=512):
    r, f = h.shape
    d = wd.shape[1]

    def body(i_ref, h_ref, w_ref, *rest):
        def rows(m):
            v = mm(h_ref[m, :], w_ref[...])
            rest[-1][m, :] = v if add is None else v + rest[0][m, :]

        row_loop(r, 256, rows)

    o = spec((r, tn), lambda n, i: (0, n))
    more = () if add is None else (add,)
    return call(
        body, core, (d // tn,),
        [spec((r, f), lambda n, i: (0, 0), True), spec((f, tn), lambda n, i: (0, n))] + [o] * len(more),
        [(o, (r, d), f32)], (h, wd) + more, 2 * r * d * f,
    )[0]


def k_g(core, slot, dy, wd, a, b, keep, tn=512):
    r, d = dy.shape
    f = wd.shape[0]
    steps = pl.cdiv(f, tn)
    n_in = 5 + len(keep)

    def body(*refs):
        _, dy_ref, w_ref, a_ref, b_ref = refs[:5]
        da_ref, db_ref, daall_ref, dball_ref, dyall_ref, sem = refs[n_in:]
        n = pl.program_id(0)
        keep_dy = pltpu.make_async_copy(dy_ref, dyall_ref.at[pl.ds(slot * r, r), :], sem)

        @pl.when(n == 0)
        def _():
            keep_dy.start()

        def rows(m):
            g = dg(dy_ref[m, :], w_ref[...], NT)
            a = a_ref[m, :]
            b = b_ref[m, :]
            sig = jax.nn.sigmoid(a)
            da = (g * b * sig * (1.0 + a * (1.0 - sig))).astype(bf)
            db = (g * (a * sig)).astype(bf)
            da_ref[m, :] = da
            db_ref[m, :] = db
            daall_ref[m, :] = da
            dball_ref[m, :] = db

        row_loop(r, 256, rows)

        @pl.when(n == steps - 1)
        def _():
            keep_dy.wait()

    o = spec((r, tn), lambda n, i: (0, n))
    oall = spec((r, tn), lambda n, i: (slot, n))
    return call(
        body, core, (steps,),
        [spec((r, d), lambda n, i: (0, 0), True), spec((tn, d), lambda n, i: (n, 0)), o, o] + [ANY] * len(keep),
        [(o, (r, f), bf), (o, (r, f), bf), (oall, (4 * r, f), bf), (oall, (4 * r, f), bf), (ANY, (4 * r, d), bf)],
        (dy, wd, a, b) + tuple(keep), 2 * r * d * f,
        scratch=[pltpu.SemaphoreType.DMA], aliases={5: 2, 6: 3, 7: 4} if keep else None,
    )


def k_dx(core, da, db, wg, wu, add=None, pieces=1, tn=512):
    r, f = da.shape
    d = wg.shape[0]
    rp = r // pieces
    more = () if add is None else (add,)

    def body(i_ref, da_ref, db_ref, wg_ref, wu_ref, *rest):
        outs = rest[len(more):]

        def rows(m, o_ref, mo):
            v = dg(da_ref[m, :], wg_ref[...], NT) + dg(db_ref[m, :], wu_ref[...], NT)
            o_ref[mo, :] = v if add is None else v + rest[0][m, :].astype(f32)

        if pieces == 1:
            row_loop(r, 256, lambda m: rows(m, outs[0], m))
        else:
            for p in range(pieces):
                rows(slice(p * rp, (p + 1) * rp), outs[p], slice(0, rp))

    w = spec((tn, f), lambda n, i: (n, 0))
    hs = spec((r, f), lambda n, i: (0, 0), True)
    return call(
        body, core, (d // tn,),
        [hs, hs, w, w] + [spec((r, tn), lambda n, i: (0, n))] * len(more),
        [(spec((rp, tn), lambda n, i: (0, n)), (rp, d), f32)] * pieces,
        (da, db, wg, wu) + more, 4 * r * d * f,
    )


def k_dw(core, x, xo, d, do, tm=1280, tn=512):
    t, f = d.shape
    hd = x.shape[1] // 2
    nt = hd // tm

    def body(i_ref, x_ref, xo_ref, d_ref, do_ref, o_ref):
        def cols(m):
            o_ref[m, :] = dg(x_ref[:, m], d_ref[...], TN) + dg(xo_ref[:, m], do_ref[...], TN)

        row_loop(tm, 256, cols)

    xs = spec((t, tm), lambda n, m, i: (0, m + i[0] * nt))
    ds = spec((t, tn), lambda n, m, i: (0, n))
    return call(
        body, core, (pl.cdiv(f, tn), nt), [xs, xs, ds, ds],
        [(spec((tm, tn), lambda n, m, i: (m, n)), (hd, f), f32)], (x, xo, d, do), 4 * t * hd * f,
    )[0]


def k_dwd(core, h, ho, dy, dyo, tm=1152, tn=512):
    t, f = h.shape
    hd = dy.shape[1] // 2
    nt = hd // tn

    def body(i_ref, h_ref, ho_ref, d_ref, do_ref, o_ref):
        def cols(m):
            o_ref[m, :] = dg(h_ref[:, m], d_ref[...], TN) + dg(ho_ref[:, m], do_ref[...], TN)

        row_loop(tm, 384, cols)

    hs = spec((t, tm), lambda n, m, i: (0, m))
    ds = spec((t, tn), lambda n, m, i: (0, n + i[0] * nt))
    return call(
        body, core, (nt, f // tm), [hs, hs, ds, ds],
        [(spec((tm, tn), lambda n, m, i: (m, n)), (f, hd), f32)], (h, ho, dy, dyo), 4 * t * hd * f,
    )[0]


def k_add(core, u, v, tr=96):
    r, d = u.shape

    def body(i_ref, u_ref, v_ref, o_ref):
        o_ref[...] = u_ref[...] + v_ref[...]

    o = spec((tr, d), lambda n, i: (n, 0))
    return call(body, core, (r // tr,), [o, o], [(o, (r, d), f32)], (u, v), r * d)[0]


def k_fin(core, p, u, v, keep, tr=64):
    r, d = u.shape
    n0 = p * v.shape[0] // tr

    def body(i_ref, u_ref, v_ref, *rest):
        rest[-1][...] = (u_ref[...] + v_ref[...]).astype(bf)

    o = spec((tr, d), lambda n, i: (n0 + n, 0))
    return call(
        body, core, (v.shape[0] // tr,), [o, spec((tr, d), lambda n, i: (n, 0))] + [ANY] * len(keep),
        [(o, (r, d), bf)], (u, v) + tuple(keep), r * d, aliases={3: 0} if keep else None,
    )[0]


def solution(mesh):
    ny = mesh.shape["tp"]
    rows = P(("dp", "tp"), None)
    wsp = P("dp", "tp")
    dsp = P("tp", "dp")
    axes = ("tp", "dp")

    def pairs(first):
        out = []
        for j in range(ny):
            for c in range(2):
                bit = 1 if (c == 0) == first else 2
                out.append((j * 2 + c, (j ^ bit) * 2 + c))
        return out

    p1, p2 = pairs(True), pairs(False)

    def to1(v):
        return lax.ppermute(v, axes, p1)

    def to2(v):
        return lax.ppermute(v, axes, p2)

    def swap(v):
        return lax.ppermute(v, "dp", [(0, 1), (1, 0)])

    def layer(x, wg, wu, wd, dy):
        i = lax.axis_index("dp").astype(jnp.int32).reshape(1)
        x1, x2 = to1(x), to2(x)
        dy2 = to2(dy)
        wgo, wuo, wdo = swap(wg), swap(wu), swap(wd)
        xd = to1(x2)
        dy1 = to1(dy)
        dyd = to1(dy2)

        a0, b0, h0, hall, xall, wgc, wuc = k_fwd0(i, x, wg, wgo, wu, wuo)
        y0, wdc = k_y0(i, h0, wd, wdo)
        a1, b1, h1, hall, xall = k_fwd(i, 1, x1, wgc, wuc, hall, xall)
        a2, b2, h2, hall, xall = k_fwd(i, 2, x2, wgc, wuc, hall, xall)
        a3, b3, h3, hall, xall = k_fwd(i, 3, xd, wgc, wuc, hall, xall)
        y1 = k_y(i, h1, wdc)
        y3 = k_y(i, h3, wdc)
        ra = to1(y3)
        r1 = to1(y1)
        y2 = k_y(i, h2, wdc, ra)
        r2 = to2(y2)

        def bwd(slot, v, a, b, keep):
            return k_g(i, slot, v, wdc, a, b, keep)

        da0, db0, *alls = bwd(0, dy, a0, b0, ())
        da1, db1, *alls = bwd(1, dy1, a1, b1, alls)
        da2, db2, *alls = bwd(2, dy2, a2, b2, alls)
        da3, db3, *alls = bwd(3, dyd, a3, b3, alls)
        daall, dball, dyall = alls
        z0 = k_dx(i, da0, db0, wgc, wuc, add=dy)[0]
        z1 = k_dx(i, da1, db1, wgc, wuc)[0]
        z3 = k_dx(i, da3, db3, wgc, wuc)[0]
        sa = to1(z3)
        s1 = to1(z1)
        z2 = k_dx(i, da2, db2, wgc, wuc, add=sa, pieces=4)
        s2 = [to2(z2[p]) for p in range(4)]

        xallo, hallo = swap(xall), swap(hall)
        dyallo, daallo, dballo = swap(dyall), swap(daall), swap(dball)
        dwd = k_dwd(i, hall, hallo, dyall, dyallo)
        dwg = k_dw(i, xall, xallo, daall, daallo)
        dwu = k_dw(i, xall, xallo, dball, dballo)

        y = (x.astype(f32) + y0 + r1 + r2).astype(bf)
        pre = k_add(i, z0, s1)
        dx = ()
        for p in range(4):
            dx = (k_fin(i, p, pre, s2[p], dx),)
        return y, dx[0], dwg, dwu, dwd

    return jax.shard_map(layer, mesh=mesh, in_specs=(rows, wsp, wsp, dsp, rows), out_specs=(rows, rows, wsp, wsp, dsp), check_vma=False)
```

```python
import jax
import jax.numpy as jnp
from jax import lax
from jax.experimental import pallas as pl
from jax.experimental.pallas import tpu as pltpu
from jax.sharding import PartitionSpec as P


f32 = jnp.float32
bf = jnp.bfloat16
NT = (((1,), (1,)), ((), ()))
TN = (((0,), (0,)), ((), ()))
VMEM = 62 * 1024 * 1024
ONE = pl.Buffered(1)
ANY = pl.BlockSpec(memory_space=pl.ANY)


def mm(u, v):
    return jnp.dot(u, v, preferred_element_type=f32)


def dg(u, v, dims):
    return lax.dot_general(u, v, dims, preferred_element_type=f32)


def sds(shape, dtype):
    return jax.ShapeDtypeStruct(shape, dtype)


def spec(shape, index, once=False):
    if once:
        return pl.BlockSpec(shape, index, pipeline_mode=ONE)
    return pl.BlockSpec(shape, index)


def row_loop(rows, step, fn):
    def trip(m, carry):
        fn(pl.ds(pl.multiple_of(m * step, step), step))
        return carry

    lax.fori_loop(0, rows // step, trip, 0)


def call(body, core, grid, ins, outs, args, flops, scratch=(), aliases=None):
    moved = sum(a.size * a.dtype.itemsize for a in args)
    return pl.pallas_call(
        body,
        grid_spec=pltpu.PrefetchScalarGridSpec(
            num_scalar_prefetch=1, grid=grid, in_specs=list(ins), out_specs=[o[0] for o in outs], scratch_shapes=list(scratch)
        ),
        out_shape=[sds(o[1], o[2]) for o in outs],
        input_output_aliases=aliases or {},
        compiler_params=pltpu.CompilerParams(dimension_semantics=("arbitrary",) * len(grid), vmem_limit_bytes=VMEM),
        cost_estimate=pl.CostEstimate(flops=int(flops), bytes_accessed=int(moved), transcendentals=0),
    )(core, *args)


def silu_h(a, b):
    return (a * jax.nn.sigmoid(a) * b).astype(bf)


def k_fwd0(core, x, wg, wgo, wu, wuo, tn=512):
    r, d = x.shape
    hd, f = wg.shape
    steps = pl.cdiv(f, tn)
    last = f - (steps - 1) * tn

    def body(i_ref, x_ref, wg_ref, wgo_ref, wu_ref, wuo_ref, a_ref, b_ref, h_ref, hall_ref, xall_ref, wgc_ref, wuc_ref, sem, wsem):
        n = pl.program_id(0)
        s = pl.multiple_of(i_ref[0] * hd, 128)
        o = pl.multiple_of((1 - i_ref[0]) * hd, 128)
        keep_x = pltpu.make_async_copy(x_ref, xall_ref.at[pl.ds(0, r), :], sem)

        def copies(width):
            c = pl.ds(pl.multiple_of(n * tn, 128), width)
            moves = ((wg_ref, wgc_ref, s), (wgo_ref, wgc_ref, o), (wu_ref, wuc_ref, s), (wuo_ref, wuc_ref, o))
            return [
                pltpu.make_async_copy(u.at[:, pl.ds(0, width)], v.at[pl.ds(q, hd), c], wsem.at[k])
                for k, (u, v, q) in enumerate(moves)
            ]

        @pl.when(n == 0)
        def _():
            keep_x.start()

        @pl.when(n < steps - 1)
        def _():
            for c in copies(tn):
                c.start()

        @pl.when(n == steps - 1)
        def _():
            for c in copies(last):
                c.start()

        def rows(m):
            xs = x_ref[m, pl.ds(s, hd)]
            xo = x_ref[m, pl.ds(o, hd)]
            a = mm(xs, wg_ref[...]) + mm(xo, wgo_ref[...])
            b = mm(xs, wu_ref[...]) + mm(xo, wuo_ref[...])
            a_ref[m, :] = a
            b_ref[m, :] = b
            h = silu_h(a, b)
            h_ref[m, :] = h
            hall_ref[m, :] = h

        row_loop(r, 256, rows)

        @pl.when(n < steps - 1)
        def _():
            for c in copies(tn):
                c.wait()

        @pl.when(n == steps - 1)
        def _():
            for c in copies(last):
                c.wait()
            keep_x.wait()

    w = spec((hd, tn), lambda n, i: (0, n))
    o = spec((r, tn), lambda n, i: (0, n))
    return call(
        body, core, (steps,),
        [spec((r, d), lambda n, i: (0, 0), True), w, w, w, w],
        [(o, (r, f), f32), (o, (r, f), f32), (o, (r, f), bf), (o, (4 * r, f), bf), (ANY, (4 * r, d), bf),
         (ANY, (d, f), bf), (ANY, (d, f), bf)],
        (x, wg, wgo, wu, wuo), 4 * r * d * f,
        scratch=[pltpu.SemaphoreType.DMA, pltpu.SemaphoreType.DMA((4,))],
    )


def k_fwd(core, slot, x, wg, wu, hall, xall, tn=512):
    r, d = x.shape
    f = wg.shape[1]
    steps = pl.cdiv(f, tn)

    def body(i_ref, x_ref, wg_ref, wu_ref, hin_ref, xin_ref, a_ref, b_ref, h_ref, hall_ref, xall_ref, sem):
        n = pl.program_id(0)
        keep_x = pltpu.make_async_copy(x_ref, xall_ref.at[pl.ds(slot * r, r), :], sem)

        @pl.when(n == 0)
        def _():
            keep_x.start()

        def rows(m):
            a = mm(x_ref[m, :], wg_ref[...])
            b = mm(x_ref[m, :], wu_ref[...])
            a_ref[m, :] = a
            b_ref[m, :] = b
            h = silu_h(a, b)
            h_ref[m, :] = h
            hall_ref[m, :] = h

        row_loop(r, 256, rows)

        @pl.when(n == steps - 1)
        def _():
            keep_x.wait()

    w = spec((d, tn), lambda n, i: (0, n))
    o = spec((r, tn), lambda n, i: (0, n))
    return call(
        body, core, (steps,),
        [spec((r, d), lambda n, i: (0, 0), True), w, w, ANY, ANY],
        [(o, (r, f), f32), (o, (r, f), f32), (o, (r, f), bf),
         (spec((r, tn), lambda n, i: (slot, n)), (4 * r, f), bf), (ANY, (4 * r, d), bf)],
        (x, wg, wu, hall, xall), 4 * r * d * f,
        scratch=[pltpu.SemaphoreType.DMA], aliases={4: 3, 5: 4},
    )


def k_y2(core, h, wd, hr, ws, res=None, tn=512):
    r, f = h.shape
    d = wd.shape[1]
    ka = ws[0].shape[0]
    nt = d // 2 // tn

    def body(i_ref, h_ref, w_ref, hr_ref, *rest):
        n = pl.program_id(0)
        own = (n < nt) == (i_ref[0] == 0)
        o_ref = rest[-1]

        def part(ua, ub):
            def rows(m):
                v = mm(h_ref[m, :], w_ref[...]) + (mm(hr_ref[m, :ka], ua[...]) + mm(hr_ref[m, ka:], ub[...]))
                if res is not None:
                    v = (rest[4][m, :].astype(f32) + v + rest[5][m, :]).astype(bf)
                o_ref[m, :] = v

            row_loop(r, 256, rows)

        @pl.when(own)
        def _():
            part(rest[0], rest[1])

        @pl.when(jnp.logical_not(own))
        def _():
            part(rest[2], rest[3])

    o = spec((r, tn), lambda n, i: (0, n))
    hs = spec((r, f), lambda n, i: (0, 0), True)

    def part_spec(k, other):
        return spec((k, tn), lambda n, i: (0, jnp.clip(n - ((1 - i[0]) if other else i[0]) * nt, 0, nt - 1)))

    more = () if res is None else tuple(res)
    return call(
        body, core, (2 * nt,),
        [hs, spec((f, tn), lambda n, i: (0, n)), hs]
        + [part_spec(ka, False), part_spec(f - ka, False), part_spec(ka, True), part_spec(f - ka, True)] + [o] * len(more),
        [(o, (r, d), f32 if res is None else bf)], (h, wd, hr) + tuple(ws) + more, 4 * r * d * f,
    )[0]


def grads(g, a, b):
    sig = jax.nn.sigmoid(a)
    return (g * b * sig * (1.0 + a * (1.0 - sig))).astype(bf), (g * (a * sig)).astype(bf)


def k_g0(core, dy, wd, wdo, a, b, tn=512):
    r, d = dy.shape
    f, hd = wd.shape
    steps = pl.cdiv(f, tn)
    last = f - (steps - 1) * tn

    def body(i_ref, dy_ref, w_ref, wo_ref, a_ref, b_ref, daall_ref, dball_ref, dyall_ref, wc_ref, sem, wsem):
        n = pl.program_id(0)
        s = pl.multiple_of(i_ref[0] * hd, 128)
        o = pl.multiple_of((1 - i_ref[0]) * hd, 128)
        keep_dy = pltpu.make_async_copy(dy_ref, dyall_ref.at[pl.ds(0, r), :], sem)

        def copies(height):
            c = pl.ds(pl.multiple_of(n * tn, 128), height)
            return [
                pltpu.make_async_copy(u.at[pl.ds(0, height), :], wc_ref.at[c, pl.ds(q, hd)], wsem.at[k])
                for k, (u, q) in enumerate(((w_ref, s), (wo_ref, o)))
            ]

        @pl.when(n == 0)
        def _():
            keep_dy.start()

        @pl.when(n < steps - 1)
        def _():
            for c in copies(tn):
                c.start()

        @pl.when(n == steps - 1)
        def _():
            for c in copies(last):
                c.start()

        def rows(m):
            g = dg(dy_ref[m, pl.ds(s, hd)], w_ref[...], NT) + dg(dy_ref[m, pl.ds(o, hd)], wo_ref[...], NT)
            daall_ref[m, :], dball_ref[m, :] = grads(g, a_ref[m, :], b_ref[m, :])

        row_loop(r, 256, rows)

        @pl.when(n < steps - 1)
        def _():
            for c in copies(tn):
                c.wait()

        @pl.when(n == steps - 1)
        def _():
            for c in copies(last):
                c.wait()
            keep_dy.wait()

    o = spec((r, tn), lambda n, i: (0, n))
    w = spec((tn, hd), lambda n, i: (n, 0))
    return call(
        body, core, (steps,),
        [spec((r, d), lambda n, i: (0, 0), True), w, w, o, o],
        [(o, (4 * r, f), bf), (o, (4 * r, f), bf), (ANY, (4 * r, d), bf), (ANY, (f, d), bf)],
        (dy, wd, wdo, a, b), 2 * r * d * f,
        scratch=[pltpu.SemaphoreType.DMA, pltpu.SemaphoreType.DMA((2,))],
    )


def k_g(core, slot, dy, wd, a, b, keep, after=(), tn=512):
    r, d = dy.shape
    f = wd.shape[0]
    steps = pl.cdiv(f, tn)
    n_in = 8 + len(after)

    def body(*refs):
        _, dy_ref, w_ref, a_ref, b_ref = refs[:5]
        daall_ref, dball_ref, dyall_ref, sem = refs[n_in:]
        n = pl.program_id(0)
        keep_dy = pltpu.make_async_copy(dy_ref, dyall_ref.at[pl.ds(slot * r, r), :], sem)

        @pl.when(n == 0)
        def _():
            keep_dy.start()

        def rows(m):
            g = dg(dy_ref[m, :], w_ref[...], NT)
            daall_ref[m, :], dball_ref[m, :] = grads(g, a_ref[m, :], b_ref[m, :])

        row_loop(r, 256, rows)

        @pl.when(n == steps - 1)
        def _():
            keep_dy.wait()

    o = spec((r, tn), lambda n, i: (0, n))
    oall = spec((r, tn), lambda n, i: (slot, n))
    return call(
        body, core, (steps,),
        [spec((r, d), lambda n, i: (0, 0), True), spec((tn, d), lambda n, i: (n, 0)), o, o] + [ANY] * (3 + len(after)),
        [(oall, (4 * r, f), bf), (oall, (4 * r, f), bf), (ANY, (4 * r, d), bf)],
        (dy, wd, a, b) + tuple(keep) + tuple(after), 2 * r * d * f,
        scratch=[pltpu.SemaphoreType.DMA], aliases={5: 0, 6: 1, 7: 2},
    )


def k_dx(core, slot, daall, dball, wg, wu, add=None, tn=512):
    f = daall.shape[1]
    r = daall.shape[0] // 4
    d = wg.shape[0]
    more = () if add is None else (add,)

    def body(i_ref, da_ref, db_ref, wg_ref, wu_ref, *rest):
        def rows(m):
            v = dg(da_ref[m, :], wg_ref[...], NT) + dg(db_ref[m, :], wu_ref[...], NT)
            rest[-1][m, :] = v if add is None else v + rest[0][m, :].astype(f32)

        row_loop(r, 256, rows)

    w = spec((tn, f), lambda n, i: (n, 0))
    hs = spec((r, f), lambda n, i: (slot(i[0]), 0), True)
    o = spec((r, tn), lambda n, i: (0, n))
    return call(
        body, core, (d // tn,), [hs, hs, w, w] + [o] * len(more),
        [(o, (r, d), f32)], (daall, dball, wg, wu) + more, 4 * r * d * f,
    )[0]


def k_dw(core, x, xo, d, do, tm=1280, tn=512):
    t, f = d.shape
    hd = x.shape[1] // 2
    nt = hd // tm

    def body(i_ref, x_ref, xo_ref, d_ref, do_ref, o_ref):
        def cols(m):
            o_ref[m, :] = dg(x_ref[:, m], d_ref[...], TN) + dg(xo_ref[:, m], do_ref[...], TN)

        row_loop(tm, 256, cols)

    xs = spec((t, tm), lambda n, m, i: (0, m + i[0] * nt))
    ds = spec((t, tn), lambda n, m, i: (0, n))
    return call(
        body, core, (pl.cdiv(f, tn), nt), [xs, xs, ds, ds],
        [(spec((tm, tn), lambda n, m, i: (m, n)), (hd, f), f32)], (x, xo, d, do), 4 * t * hd * f,
    )[0]


def k_dwd(core, h, ho, dy, dyo, tm=1152, tn=512):
    t, f = h.shape
    hd = dy.shape[1] // 2
    nt = hd // tn

    def body(i_ref, h_ref, ho_ref, d_ref, do_ref, o_ref):
        def cols(m):
            o_ref[m, :] = dg(h_ref[:, m], d_ref[...], TN) + dg(ho_ref[:, m], do_ref[...], TN)

        row_loop(tm, 384, cols)

    hs = spec((t, tm), lambda n, m, i: (0, m))
    ds = spec((t, tn), lambda n, m, i: (0, n + i[0] * nt))
    return call(
        body, core, (nt, f // tm), [hs, hs, ds, ds],
        [(spec((tm, tn), lambda n, m, i: (m, n)), (f, hd), f32)], (h, ho, dy, dyo), 4 * t * hd * f,
    )[0]


def k_add(core, u, v, pieces=1, tn=512):
    r, d = u.shape
    rp = r // pieces

    def body(i_ref, u_ref, v_ref, *outs):
        for p, o_ref in enumerate(outs):
            m = slice(p * rp, (p + 1) * rp)
            o_ref[...] = u_ref[m, :] + v_ref[m, :]

    s = spec((r, tn), lambda n, i: (0, n))
    o = spec((rp, tn), lambda n, i: (0, n))
    return call(body, core, (d // tn,), [s, s], [(o, (rp, d), f32)] * pieces, (u, v), r * d)


def k_fin(core, p, u, v, keep, tr=64):
    r, d = u.shape
    n0 = p * v.shape[0] // tr

    def body(i_ref, u_ref, v_ref, *rest):
        rest[-1][...] = (u_ref[...] + v_ref[...]).astype(bf)

    o = spec((tr, d), lambda n, i: (n0 + n, 0))
    return call(
        body, core, (v.shape[0] // tr,), [o, spec((tr, d), lambda n, i: (n, 0))] + [ANY] * len(keep),
        [(o, (r, d), bf)], (u, v) + tuple(keep), r * d, aliases={3: 0} if keep else None,
    )[0]


def solution(mesh):
    ny = mesh.shape["tp"]
    rows = P(("dp", "tp"), None)
    wsp = P("dp", "tp")
    dsp = P("tp", "dp")
    axes = ("tp", "dp")

    def hop(v, bit0, bit1):
        pairs = [(j * 2 + c, (j ^ b) * 2 + c) for j in range(ny) for c, b in enumerate((bit0, bit1))]
        return lax.ppermute(v, axes, pairs)

    def swap(v):
        return lax.ppermute(v, "dp", [(0, 1), (1, 0)])

    def layer(x, wg, wu, wd, dy):
        i = lax.axis_index("dp").astype(jnp.int32).reshape(1)
        ka = 1792
        qa = 304
        xX, xY = hop(x, 1, 1), hop(x, 2, 2)
        dyX, dyY = hop(dy, 1, 1), hop(dy, 2, 2)
        wgo, wuo, wdo = swap(wg), swap(wu), swap(wd)
        wXa, wXb = hop(wd[:ka], 1, 1), hop(wd[ka:], 1, 1)
        xD = hop(xX, 2, 2)
        dyDa = hop(jnp.where(i[0] == 0, dyY[:qa], dyX[:qa]), 1, 2)
        dyDb = hop(dyX[qa:], 2, 2)
        dyD = jnp.concatenate([dyDa, dyDb], axis=0)
        wX = (wXa, wXb, swap(wXa), swap(wXb))

        a0, b0, h0, hall, xall, wgc, wuc = k_fwd0(i, x, wg, wgo, wu, wuo)
        *alls, wdc = k_g0(i, dy, wd, wdo, a0, b0)
        a1, b1, h1, hall, xall = k_fwd(i, 1, xX, wgc, wuc, hall, xall)
        a2, b2, h2, hall, xall = k_fwd(i, 2, xY, wgc, wuc, hall, xall)
        a3, b3, h3, hall, xall = k_fwd(i, 3, xD, wgc, wuc, hall, xall)

        alls = k_g(i, 1, dyX, wdc, a1, b1, alls)
        alls = k_g(i, 2, dyY, wdc, a2, b2, alls)
        z1 = k_dx(i, lambda c: 1 + c, alls[0], alls[1], wgc, wuc)
        s1 = hop(z1, 1, 2)
        z0 = k_dx(i, lambda c: 0, alls[0], alls[1], wgc, wuc, add=dy)
        daall, dball, dyall = k_g(i, 3, dyD, wdc, a3, b3, alls, (z0, z1))
        z3 = k_dx(i, lambda c: 3, daall, dball, wgc, wuc)
        sa = hop(z3, 1, 2)
        z2 = k_dx(i, lambda c: 2 - c, daall, dball, wgc, wuc)
        s2 = k_add(i, z2, sa, pieces=4)
        s2 = [hop(s2[p], 2, 1) for p in range(4)]

        hDr, hXr = hop(h3, 1, 1), hop(h1, 1, 1)
        yYr = hop(k_y2(i, h2, wdc, hDr, wX), 2, 2)
        y = k_y2(i, h0, wdc, hXr, wX, (x, yYr))

        xallo, hallo = swap(xall), swap(hall)
        dyallo, daallo, dballo = swap(dyall), swap(daall), swap(dball)
        dwd = k_dwd(i, hall, hallo, dyall, dyallo)
        dwg = k_dw(i, xall, xallo, daall, daallo)
        dwu = k_dw(i, xall, xallo, dball, dballo)

        pre = k_add(i, z0, s1)[0]
        dx = ()
        for p in range(4):
            dx = (k_fin(i, p, pre, s2[p], dx),)
        return y, dx[0], dwg, dwu, dwd

    return jax.shard_map(layer, mesh=mesh, in_specs=(rows, wsp, wsp, dsp, rows), out_specs=(rows, rows, wsp, wsp, dsp), check_vma=False)
```

```python
import jax
import jax.numpy as jnp
from jax import lax
from jax.experimental import pallas as pl
from jax.experimental.pallas import tpu as pltpu
from jax.sharding import PartitionSpec as P


f32 = jnp.float32
bf = jnp.bfloat16
NT = (((1,), (1,)), ((), ()))
TN = (((0,), (0,)), ((), ()))
VMEM = 62 * 1024 * 1024
ONE = pl.Buffered(1)
ANY = pl.BlockSpec(memory_space=pl.ANY)


def mm(u, v):
    return jnp.dot(u, v, preferred_element_type=f32)


def dg(u, v, dims):
    return lax.dot_general(u, v, dims, preferred_element_type=f32)


def sds(shape, dtype):
    return jax.ShapeDtypeStruct(shape, dtype)


def spec(shape, index, once=False):
    if once:
        return pl.BlockSpec(shape, index, pipeline_mode=ONE)
    return pl.BlockSpec(shape, index)


def row_loop(rows, step, fn):
    def trip(m, carry):
        fn(pl.ds(pl.multiple_of(m * step, step), step))
        return carry

    lax.fori_loop(0, rows // step, trip, 0)


def call(body, core, grid, ins, outs, args, flops, scratch=(), aliases=None):
    moved = sum(a.size * a.dtype.itemsize for a in args)
    return pl.pallas_call(
        body,
        grid_spec=pltpu.PrefetchScalarGridSpec(
            num_scalar_prefetch=1, grid=grid, in_specs=list(ins), out_specs=[o[0] for o in outs], scratch_shapes=list(scratch)
        ),
        out_shape=[sds(o[1], o[2]) for o in outs],
        input_output_aliases=aliases or {},
        compiler_params=pltpu.CompilerParams(dimension_semantics=("arbitrary",) * len(grid), vmem_limit_bytes=VMEM),
        cost_estimate=pl.CostEstimate(flops=int(flops), bytes_accessed=int(moved), transcendentals=0),
    )(core, *args)


def silu_h(a, b):
    return (a * jax.nn.sigmoid(a) * b).astype(bf)


def k_fwd0(core, x, wg, wgo, wu, wuo, tn=512):
    r, d = x.shape
    hd, f = wg.shape
    steps = pl.cdiv(f, tn)
    last = f - (steps - 1) * tn

    def body(i_ref, x_ref, wg_ref, wgo_ref, wu_ref, wuo_ref, a_ref, b_ref, h_ref, hall_ref, xall_ref, wgc_ref, wuc_ref, sem, wsem):
        n = pl.program_id(0)
        s = pl.multiple_of(i_ref[0] * hd, 128)
        o = pl.multiple_of((1 - i_ref[0]) * hd, 128)
        keep_x = pltpu.make_async_copy(x_ref, xall_ref.at[pl.ds(0, r), :], sem)

        def copies(width):
            c = pl.ds(pl.multiple_of(n * tn, 128), width)
            moves = ((wg_ref, wgc_ref, s), (wgo_ref, wgc_ref, o), (wu_ref, wuc_ref, s), (wuo_ref, wuc_ref, o))
            return [
                pltpu.make_async_copy(u.at[:, pl.ds(0, width)], v.at[pl.ds(q, hd), c], wsem.at[k])
                for k, (u, v, q) in enumerate(moves)
            ]

        @pl.when(n == 0)
        def _():
            keep_x.start()

        @pl.when(n < steps - 1)
        def _():
            for c in copies(tn):
                c.start()

        @pl.when(n == steps - 1)
        def _():
            for c in copies(last):
                c.start()

        def rows(m):
            xs = x_ref[m, pl.ds(s, hd)]
            xo = x_ref[m, pl.ds(o, hd)]
            a = mm(xs, wg_ref[...]) + mm(xo, wgo_ref[...])
            b = mm(xs, wu_ref[...]) + mm(xo, wuo_ref[...])
            a_ref[m, :] = a
            b_ref[m, :] = b
            h = silu_h(a, b)
            h_ref[m, :] = h
            hall_ref[m, :] = h

        row_loop(r, 256, rows)

        @pl.when(n < steps - 1)
        def _():
            for c in copies(tn):
                c.wait()

        @pl.when(n == steps - 1)
        def _():
            for c in copies(last):
                c.wait()
            keep_x.wait()

    w = spec((hd, tn), lambda n, i: (0, n))
    o = spec((r, tn), lambda n, i: (0, n))
    return call(
        body, core, (steps,),
        [spec((r, d), lambda n, i: (0, 0), True), w, w, w, w],
        [(o, (r, f), f32), (o, (r, f), f32), (o, (r, f), bf), (o, (4 * r, f), bf), (ANY, (4 * r, d), bf),
         (ANY, (d, f), bf), (ANY, (d, f), bf)],
        (x, wg, wgo, wu, wuo), 4 * r * d * f,
        scratch=[pltpu.SemaphoreType.DMA, pltpu.SemaphoreType.DMA((4,))],
    )


def k_fwd(core, slot, x, wg, wu, hall, xall, tn=512):
    r, d = x.shape
    f = wg.shape[1]
    steps = pl.cdiv(f, tn)

    def body(i_ref, x_ref, wg_ref, wu_ref, hin_ref, xin_ref, a_ref, b_ref, h_ref, hall_ref, xall_ref, sem):
        n = pl.program_id(0)
        keep_x = pltpu.make_async_copy(x_ref, xall_ref.at[pl.ds(slot * r, r), :], sem)

        @pl.when(n == 0)
        def _():
            keep_x.start()

        def rows(m):
            a = mm(x_ref[m, :], wg_ref[...])
            b = mm(x_ref[m, :], wu_ref[...])
            a_ref[m, :] = a
            b_ref[m, :] = b
            h = silu_h(a, b)
            h_ref[m, :] = h
            hall_ref[m, :] = h

        row_loop(r, 256, rows)

        @pl.when(n == steps - 1)
        def _():
            keep_x.wait()

    w = spec((d, tn), lambda n, i: (0, n))
    o = spec((r, tn), lambda n, i: (0, n))
    return call(
        body, core, (steps,),
        [spec((r, d), lambda n, i: (0, 0), True), w, w, ANY, ANY],
        [(o, (r, f), f32), (o, (r, f), f32), (o, (r, f), bf),
         (spec((r, tn), lambda n, i: (slot, n)), (4 * r, f), bf), (ANY, (4 * r, d), bf)],
        (x, wg, wu, hall, xall), 4 * r * d * f,
        scratch=[pltpu.SemaphoreType.DMA], aliases={4: 3, 5: 4},
    )


def k_y2(core, h, wd, hr, ws, res=None, tn=512):
    r, f = h.shape
    d = wd.shape[1]
    ka = ws[0].shape[0]
    nt = d // 2 // tn

    def body(i_ref, h_ref, w_ref, hr_ref, *rest):
        n = pl.program_id(0)
        own = (n < nt) == (i_ref[0] == 0)
        o_ref = rest[-1]

        def part(ua, ub):
            def rows(m):
                v = mm(h_ref[m, :], w_ref[...]) + (mm(hr_ref[m, :ka], ua[...]) + mm(hr_ref[m, ka:], ub[...]))
                if res is not None:
                    v = (rest[4][m, :].astype(f32) + v + rest[5][m, :]).astype(bf)
                o_ref[m, :] = v

            row_loop(r, 256, rows)

        @pl.when(own)
        def _():
            part(rest[0], rest[1])

        @pl.when(jnp.logical_not(own))
        def _():
            part(rest[2], rest[3])

    o = spec((r, tn), lambda n, i: (0, n))
    hs = spec((r, f), lambda n, i: (0, 0), True)

    def part_spec(k, other):
        return spec((k, tn), lambda n, i: (0, jnp.clip(n - ((1 - i[0]) if other else i[0]) * nt, 0, nt - 1)))

    more = () if res is None else tuple(res)
    return call(
        body, core, (2 * nt,),
        [hs, spec((f, tn), lambda n, i: (0, n)), hs]
        + [part_spec(ka, False), part_spec(f - ka, False), part_spec(ka, True), part_spec(f - ka, True)] + [o] * len(more),
        [(o, (r, d), f32 if res is None else bf)], (h, wd, hr) + tuple(ws) + more, 4 * r * d * f,
    )[0]


def grads(g, a, b):
    sig = jax.nn.sigmoid(a)
    return (g * b * sig * (1.0 + a * (1.0 - sig))).astype(bf), (g * (a * sig)).astype(bf)


def k_g0(core, dy, wd, wdo, a, b, tn=512):
    r, d = dy.shape
    f, hd = wd.shape
    steps = pl.cdiv(f, tn)
    last = f - (steps - 1) * tn

    def body(i_ref, dy_ref, w_ref, wo_ref, a_ref, b_ref, daall_ref, dball_ref, dyall_ref, wc_ref, sem, wsem):
        n = pl.program_id(0)
        s = pl.multiple_of(i_ref[0] * hd, 128)
        o = pl.multiple_of((1 - i_ref[0]) * hd, 128)
        keep_dy = pltpu.make_async_copy(dy_ref, dyall_ref.at[pl.ds(0, r), :], sem)

        def copies(height):
            c = pl.ds(pl.multiple_of(n * tn, 128), height)
            return [
                pltpu.make_async_copy(u.at[pl.ds(0, height), :], wc_ref.at[c, pl.ds(q, hd)], wsem.at[k])
                for k, (u, q) in enumerate(((w_ref, s), (wo_ref, o)))
            ]

        @pl.when(n == 0)
        def _():
            keep_dy.start()

        @pl.when(n < steps - 1)
        def _():
            for c in copies(tn):
                c.start()

        @pl.when(n == steps - 1)
        def _():
            for c in copies(last):
                c.start()

        def rows(m):
            g = dg(dy_ref[m, pl.ds(s, hd)], w_ref[...], NT) + dg(dy_ref[m, pl.ds(o, hd)], wo_ref[...], NT)
            daall_ref[m, :], dball_ref[m, :] = grads(g, a_ref[m, :], b_ref[m, :])

        row_loop(r, 256, rows)

        @pl.when(n < steps - 1)
        def _():
            for c in copies(tn):
                c.wait()

        @pl.when(n == steps - 1)
        def _():
            for c in copies(last):
                c.wait()
            keep_dy.wait()

    o = spec((r, tn), lambda n, i: (0, n))
    w = spec((tn, hd), lambda n, i: (n, 0))
    return call(
        body, core, (steps,),
        [spec((r, d), lambda n, i: (0, 0), True), w, w, o, o],
        [(o, (4 * r, f), bf), (o, (4 * r, f), bf), (ANY, (4 * r, d), bf), (ANY, (f, d), bf)],
        (dy, wd, wdo, a, b), 2 * r * d * f,
        scratch=[pltpu.SemaphoreType.DMA, pltpu.SemaphoreType.DMA((2,))],
    )


def k_g(core, slot, dy, wd, a, b, keep, after=(), tn=512):
    r, d = dy.shape
    f = wd.shape[0]
    steps = pl.cdiv(f, tn)
    n_in = 8 + len(after)

    def body(*refs):
        _, dy_ref, w_ref, a_ref, b_ref = refs[:5]
        daall_ref, dball_ref, dyall_ref, sem = refs[n_in:]
        n = pl.program_id(0)
        keep_dy = pltpu.make_async_copy(dy_ref, dyall_ref.at[pl.ds(slot * r, r), :], sem)

        @pl.when(n == 0)
        def _():
            keep_dy.start()

        def rows(m):
            g = dg(dy_ref[m, :], w_ref[...], NT)
            daall_ref[m, :], dball_ref[m, :] = grads(g, a_ref[m, :], b_ref[m, :])

        row_loop(r, 256, rows)

        @pl.when(n == steps - 1)
        def _():
            keep_dy.wait()

    o = spec((r, tn), lambda n, i: (0, n))
    oall = spec((r, tn), lambda n, i: (slot, n))
    return call(
        body, core, (steps,),
        [spec((r, d), lambda n, i: (0, 0), True), spec((tn, d), lambda n, i: (n, 0)), o, o] + [ANY] * (3 + len(after)),
        [(oall, (4 * r, f), bf), (oall, (4 * r, f), bf), (ANY, (4 * r, d), bf)],
        (dy, wd, a, b) + tuple(keep) + tuple(after), 2 * r * d * f,
        scratch=[pltpu.SemaphoreType.DMA], aliases={5: 0, 6: 1, 7: 2},
    )


def k_dx(core, slot, daall, dball, wg, wu, add=None, tn=512):
    f = daall.shape[1]
    r = daall.shape[0] // 4
    d = wg.shape[0]
    more = () if add is None else (add,)

    def body(i_ref, da_ref, db_ref, wg_ref, wu_ref, *rest):
        def rows(m):
            v = dg(da_ref[m, :], wg_ref[...], NT) + dg(db_ref[m, :], wu_ref[...], NT)
            rest[-1][m, :] = v if add is None else v + rest[0][m, :].astype(f32)

        row_loop(r, 256, rows)

    w = spec((tn, f), lambda n, i: (n, 0))
    hs = spec((r, f), lambda n, i: (slot(i[0]), 0), True)
    o = spec((r, tn), lambda n, i: (0, n))
    return call(
        body, core, (d // tn,), [hs, hs, w, w] + [o] * len(more),
        [(o, (r, d), f32)], (daall, dball, wg, wu) + more, 4 * r * d * f,
    )[0]


def k_dw(core, x, xo, d, do, tm=1280, tn=512):
    t, f = d.shape
    hd = x.shape[1] // 2
    nt = hd // tm

    def body(i_ref, x_ref, xo_ref, d_ref, do_ref, o_ref):
        def cols(m):
            o_ref[m, :] = dg(x_ref[:, m], d_ref[...], TN) + dg(xo_ref[:, m], do_ref[...], TN)

        row_loop(tm, 256, cols)

    xs = spec((t, tm), lambda n, m, i: (0, m + i[0] * nt))
    ds = spec((t, tn), lambda n, m, i: (0, n))
    return call(
        body, core, (pl.cdiv(f, tn), nt), [xs, xs, ds, ds],
        [(spec((tm, tn), lambda n, m, i: (m, n)), (hd, f), f32)], (x, xo, d, do), 4 * t * hd * f,
    )[0]


def k_dwd(core, h, ho, dy, dyo, tm=1152, tn=512):
    t, f = h.shape
    hd = dy.shape[1] // 2
    nt = hd // tn

    def body(i_ref, h_ref, ho_ref, d_ref, do_ref, o_ref):
        def cols(m):
            o_ref[m, :] = dg(h_ref[:, m], d_ref[...], TN) + dg(ho_ref[:, m], do_ref[...], TN)

        row_loop(tm, 384, cols)

    hs = spec((t, tm), lambda n, m, i: (0, m))
    ds = spec((t, tn), lambda n, m, i: (0, n + i[0] * nt))
    return call(
        body, core, (nt, f // tm), [hs, hs, ds, ds],
        [(spec((tm, tn), lambda n, m, i: (m, n)), (f, hd), f32)], (h, ho, dy, dyo), 4 * t * hd * f,
    )[0]


def k_add(core, u, v, sizes=None, tn=512):
    r, d = u.shape
    sizes = sizes or (r,)

    def body(i_ref, u_ref, v_ref, *outs):
        at = 0
        for size, o_ref in zip(sizes, outs):
            m = slice(at, at + size)
            o_ref[...] = u_ref[m, :] + v_ref[m, :]
            at += size

    s = spec((r, tn), lambda n, i: (0, n))
    outs = [(spec((size, tn), lambda n, i: (0, n)), (size, d), f32) for size in sizes]
    return call(body, core, (d // tn,), [s, s], outs, (u, v), r * d)


def k_fin(core, at, u, v, keep, tr):
    r, d = u.shape
    n0 = at // tr

    def body(i_ref, u_ref, v_ref, *rest):
        rest[-1][...] = (u_ref[...] + v_ref[...]).astype(bf)

    o = spec((tr, d), lambda n, i: (n0 + n, 0))
    return call(
        body, core, (v.shape[0] // tr,), [o, spec((tr, d), lambda n, i: (n, 0))] + [ANY] * len(keep),
        [(o, (r, d), bf)], (u, v) + tuple(keep), r * d, aliases={3: 0} if keep else None,
    )[0]


def solution(mesh):
    ny = mesh.shape["tp"]
    rows = P(("dp", "tp"), None)
    wsp = P("dp", "tp")
    dsp = P("tp", "dp")
    axes = ("tp", "dp")

    def hop(v, bit0, bit1):
        pairs = [(j * 2 + c, (j ^ b) * 2 + c) for j in range(ny) for c, b in enumerate((bit0, bit1))]
        return lax.ppermute(v, axes, pairs)

    def swap(v):
        return lax.ppermute(v, "dp", [(0, 1), (1, 0)])

    def layer(x, wg, wu, wd, dy):
        i = lax.axis_index("dp").astype(jnp.int32).reshape(1)
        ka = 1792
        qa = 312
        sizes = (448, 256, 64)
        xX, xY = hop(x, 1, 1), hop(x, 2, 2)
        dyX, dyY = hop(dy, 1, 1), hop(dy, 2, 2)
        wgo, wuo, wdo = swap(wg), swap(wu), swap(wd)
        wXa, wXb = hop(wd[:ka], 1, 1), hop(wd[ka:], 1, 1)
        xD = hop(xX, 2, 2)
        dyDa = hop(jnp.where(i[0] == 0, dyY[:qa], dyX[:qa]), 1, 2)
        dyDb = hop(dyX[qa:], 2, 2)
        dyD = jnp.concatenate([dyDa, dyDb], axis=0)
        wX = (wXa, wXb, swap(wXa), swap(wXb))

        a0, b0, h0, hall, xall, wgc, wuc = k_fwd0(i, x, wg, wgo, wu, wuo)
        *alls, wdc = k_g0(i, dy, wd, wdo, a0, b0)
        a1, b1, h1, hall, xall = k_fwd(i, 1, xX, wgc, wuc, hall, xall)
        a2, b2, h2, hall, xall = k_fwd(i, 2, xY, wgc, wuc, hall, xall)
        a3, b3, h3, hall, xall = k_fwd(i, 3, xD, wgc, wuc, hall, xall)

        alls = k_g(i, 1, dyX, wdc, a1, b1, alls)
        alls = k_g(i, 2, dyY, wdc, a2, b2, alls)
        z1 = k_dx(i, lambda c: 1 + c, alls[0], alls[1], wgc, wuc)
        s1 = hop(z1, 1, 2)
        z0 = k_dx(i, lambda c: 0, alls[0], alls[1], wgc, wuc, add=dy)
        daall, dball, dyall = k_g(i, 3, dyD, wdc, a3, b3, alls, (z0, z1))
        z3 = k_dx(i, lambda c: 3, daall, dball, wgc, wuc)
        sa = hop(z3, 1, 2)
        z2 = k_dx(i, lambda c: 2 - c, daall, dball, wgc, wuc)
        s2 = k_add(i, z2, sa, sizes)
        s2 = [hop(v, 2, 1) for v in s2]

        hDr, hXr = hop(h3, 1, 1), hop(h1, 1, 1)
        yYr = hop(k_y2(i, h2, wdc, hDr, wX), 2, 2)
        y = k_y2(i, h0, wdc, hXr, wX, (x, yYr))

        xallo, hallo = swap(xall), swap(hall)
        dyallo, daallo, dballo = swap(dyall), swap(daall), swap(dball)
        dwd = k_dwd(i, hall, hallo, dyall, dyallo)
        dwg = k_dw(i, xall, xallo, daall, daallo)
        dwu = k_dw(i, xall, xallo, dball, dballo)

        pre = k_add(i, z0, s1)[0]
        dx = ()
        for p, v in enumerate(s2):
            dx = (k_fin(i, sum(sizes[:p]), pre, v, dx, 64 if p < 2 else 32),)
        return y, dx[0], dwg, dwu, dwd

    return jax.shard_map(layer, mesh=mesh, in_specs=(rows, wsp, wsp, dsp, rows), out_specs=(rows, rows, wsp, wsp, dsp), check_vma=False)
```

```python
import jax
import jax.numpy as jnp
from jax import lax
from jax.experimental import pallas as pl
from jax.experimental.pallas import tpu as pltpu
from jax.sharding import PartitionSpec as P


f32 = jnp.float32
bf = jnp.bfloat16
NT = (((1,), (1,)), ((), ()))
TN = (((0,), (0,)), ((), ()))
VMEM = 62 * 1024 * 1024
ONE = pl.Buffered(1)
ANY = pl.BlockSpec(memory_space=pl.ANY)


def mm(u, v):
    return jnp.dot(u, v, preferred_element_type=f32)


def dg(u, v, dims):
    return lax.dot_general(u, v, dims, preferred_element_type=f32)


def sds(shape, dtype):
    return jax.ShapeDtypeStruct(shape, dtype)


def spec(shape, index, once=False):
    if once:
        return pl.BlockSpec(shape, index, pipeline_mode=ONE)
    return pl.BlockSpec(shape, index)


def row_loop(rows, step, fn):
    def trip(m, carry):
        fn(pl.ds(pl.multiple_of(m * step, step), step))
        return carry

    lax.fori_loop(0, rows // step, trip, 0)


def call(body, core, grid, ins, outs, args, flops, scratch=(), aliases=None):
    moved = sum(a.size * a.dtype.itemsize for a in args)
    return pl.pallas_call(
        body,
        grid_spec=pltpu.PrefetchScalarGridSpec(
            num_scalar_prefetch=1, grid=grid, in_specs=list(ins), out_specs=[o[0] for o in outs], scratch_shapes=list(scratch)
        ),
        out_shape=[sds(o[1], o[2]) for o in outs],
        input_output_aliases=aliases or {},
        compiler_params=pltpu.CompilerParams(dimension_semantics=("arbitrary",) * len(grid), vmem_limit_bytes=VMEM),
        cost_estimate=pl.CostEstimate(flops=int(flops), bytes_accessed=int(moved), transcendentals=0),
    )(core, *args)


def silu_h(a, b):
    return (a * jax.nn.sigmoid(a) * b).astype(bf)


def k_fwd0(core, x, wg, wgo, wu, wuo, tn=512):
    r, d = x.shape
    hd, f = wg.shape
    steps = pl.cdiv(f, tn)
    last = f - (steps - 1) * tn

    def body(i_ref, x_ref, wg_ref, wgo_ref, wu_ref, wuo_ref, a_ref, b_ref, h_ref, hall_ref, xall_ref, wgc_ref, wuc_ref, sem, wsem):
        n = pl.program_id(0)
        s = pl.multiple_of(i_ref[0] * hd, 128)
        o = pl.multiple_of((1 - i_ref[0]) * hd, 128)
        keep_x = pltpu.make_async_copy(x_ref, xall_ref.at[pl.ds(0, r), :], sem)

        def copies(width):
            c = pl.ds(pl.multiple_of(n * tn, 128), width)
            moves = ((wg_ref, wgc_ref, s), (wgo_ref, wgc_ref, o), (wu_ref, wuc_ref, s), (wuo_ref, wuc_ref, o))
            return [
                pltpu.make_async_copy(u.at[:, pl.ds(0, width)], v.at[pl.ds(q, hd), c], wsem.at[k])
                for k, (u, v, q) in enumerate(moves)
            ]

        @pl.when(n == 0)
        def _():
            keep_x.start()

        @pl.when(n < steps - 1)
        def _():
            for c in copies(tn):
                c.start()

        @pl.when(n == steps - 1)
        def _():
            for c in copies(last):
                c.start()

        def rows(m):
            xs = x_ref[m, pl.ds(s, hd)]
            xo = x_ref[m, pl.ds(o, hd)]
            a = mm(xs, wg_ref[...]) + mm(xo, wgo_ref[...])
            b = mm(xs, wu_ref[...]) + mm(xo, wuo_ref[...])
            a_ref[m, :] = a
            b_ref[m, :] = b
            h = silu_h(a, b)
            h_ref[m, :] = h
            hall_ref[m, :] = h

        row_loop(r, 256, rows)

        @pl.when(n < steps - 1)
        def _():
            for c in copies(tn):
                c.wait()

        @pl.when(n == steps - 1)
        def _():
            for c in copies(last):
                c.wait()
            keep_x.wait()

    w = spec((hd, tn), lambda n, i: (0, n))
    o = spec((r, tn), lambda n, i: (0, n))
    return call(
        body, core, (steps,),
        [spec((r, d), lambda n, i: (0, 0), True), w, w, w, w],
        [(o, (r, f), f32), (o, (r, f), f32), (o, (r, f), bf), (o, (4 * r, f), bf), (ANY, (4 * r, d), bf),
         (ANY, (d, f), bf), (ANY, (d, f), bf)],
        (x, wg, wgo, wu, wuo), 4 * r * d * f,
        scratch=[pltpu.SemaphoreType.DMA, pltpu.SemaphoreType.DMA((4,))],
    )


def k_fwd(core, slot, x, wg, wu, hall, xall, tn=512):
    r, d = x.shape
    f = wg.shape[1]
    steps = pl.cdiv(f, tn)

    def body(i_ref, x_ref, wg_ref, wu_ref, hin_ref, xin_ref, a_ref, b_ref, h_ref, hall_ref, xall_ref, sem):
        n = pl.program_id(0)
        keep_x = pltpu.make_async_copy(x_ref, xall_ref.at[pl.ds(slot * r, r), :], sem)

        @pl.when(n == 0)
        def _():
            keep_x.start()

        def rows(m):
            a = mm(x_ref[m, :], wg_ref[...])
            b = mm(x_ref[m, :], wu_ref[...])
            a_ref[m, :] = a
            b_ref[m, :] = b
            h = silu_h(a, b)
            h_ref[m, :] = h
            hall_ref[m, :] = h

        row_loop(r, 256, rows)

        @pl.when(n == steps - 1)
        def _():
            keep_x.wait()

    w = spec((d, tn), lambda n, i: (0, n))
    o = spec((r, tn), lambda n, i: (0, n))
    return call(
        body, core, (steps,),
        [spec((r, d), lambda n, i: (0, 0), True), w, w, ANY, ANY],
        [(o, (r, f), f32), (o, (r, f), f32), (o, (r, f), bf),
         (spec((r, tn), lambda n, i: (slot, n)), (4 * r, f), bf), (ANY, (4 * r, d), bf)],
        (x, wg, wu, hall, xall), 4 * r * d * f,
        scratch=[pltpu.SemaphoreType.DMA], aliases={4: 3, 5: 4},
    )


def k_y2(core, h, wd, hr, ws, res=None, tn=512):
    r, f = h.shape
    d = wd.shape[1]
    ka = ws[0].shape[0]
    nt = d // 2 // tn

    def body(i_ref, h_ref, w_ref, hr_ref, *rest):
        n = pl.program_id(0)
        own = (n < nt) == (i_ref[0] == 0)
        o_ref = rest[-1]

        def part(ua, ub):
            def rows(m):
                v = mm(h_ref[m, :], w_ref[...]) + (mm(hr_ref[m, :ka], ua[...]) + mm(hr_ref[m, ka:], ub[...]))
                if res is not None:
                    v = (rest[4][m, :].astype(f32) + v + rest[5][m, :]).astype(bf)
                o_ref[m, :] = v

            row_loop(r, 256, rows)

        @pl.when(own)
        def _():
            part(rest[0], rest[1])

        @pl.when(jnp.logical_not(own))
        def _():
            part(rest[2], rest[3])

    o = spec((r, tn), lambda n, i: (0, n))
    hs = spec((r, f), lambda n, i: (0, 0), True)

    def part_spec(k, other):
        return spec((k, tn), lambda n, i: (0, jnp.clip(n - ((1 - i[0]) if other else i[0]) * nt, 0, nt - 1)))

    more = () if res is None else tuple(res)
    return call(
        body, core, (2 * nt,),
        [hs, spec((f, tn), lambda n, i: (0, n)), hs]
        + [part_spec(ka, False), part_spec(f - ka, False), part_spec(ka, True), part_spec(f - ka, True)] + [o] * len(more),
        [(o, (r, d), f32 if res is None else bf)], (h, wd, hr) + tuple(ws) + more, 4 * r * d * f,
    )[0]


def grads(g, a, b):
    sig = jax.nn.sigmoid(a)
    return (g * b * sig * (1.0 + a * (1.0 - sig))).astype(bf), (g * (a * sig)).astype(bf)


def k_g0(core, dy, wd, wdo, a, b, tn=512):
    r, d = dy.shape
    f, hd = wd.shape
    steps = pl.cdiv(f, tn)
    last = f - (steps - 1) * tn

    def body(i_ref, dy_ref, w_ref, wo_ref, a_ref, b_ref, daall_ref, dball_ref, dyall_ref, wc_ref, sem, wsem):
        n = pl.program_id(0)
        s = pl.multiple_of(i_ref[0] * hd, 128)
        o = pl.multiple_of((1 - i_ref[0]) * hd, 128)
        keep_dy = pltpu.make_async_copy(dy_ref, dyall_ref.at[pl.ds(0, r), :], sem)

        def copies(height):
            c = pl.ds(pl.multiple_of(n * tn, 128), height)
            return [
                pltpu.make_async_copy(u.at[pl.ds(0, height), :], wc_ref.at[c, pl.ds(q, hd)], wsem.at[k])
                for k, (u, q) in enumerate(((w_ref, s), (wo_ref, o)))
            ]

        @pl.when(n == 0)
        def _():
            keep_dy.start()

        @pl.when(n < steps - 1)
        def _():
            for c in copies(tn):
                c.start()

        @pl.when(n == steps - 1)
        def _():
            for c in copies(last):
                c.start()

        def rows(m):
            g = dg(dy_ref[m, pl.ds(s, hd)], w_ref[...], NT) + dg(dy_ref[m, pl.ds(o, hd)], wo_ref[...], NT)
            daall_ref[m, :], dball_ref[m, :] = grads(g, a_ref[m, :], b_ref[m, :])

        row_loop(r, 256, rows)

        @pl.when(n < steps - 1)
        def _():
            for c in copies(tn):
                c.wait()

        @pl.when(n == steps - 1)
        def _():
            for c in copies(last):
                c.wait()
            keep_dy.wait()

    o = spec((r, tn), lambda n, i: (0, n))
    w = spec((tn, hd), lambda n, i: (n, 0))
    return call(
        body, core, (steps,),
        [spec((r, d), lambda n, i: (0, 0), True), w, w, o, o],
        [(o, (4 * r, f), bf), (o, (4 * r, f), bf), (ANY, (4 * r, d), bf), (ANY, (f, d), bf)],
        (dy, wd, wdo, a, b), 2 * r * d * f,
        scratch=[pltpu.SemaphoreType.DMA, pltpu.SemaphoreType.DMA((2,))],
    )


def k_g(core, slot, dy, wd, a, b, keep, after=(), tn=512):
    r, d = dy.shape
    f = wd.shape[0]
    steps = pl.cdiv(f, tn)
    n_in = 8 + len(after)

    def body(*refs):
        _, dy_ref, w_ref, a_ref, b_ref = refs[:5]
        daall_ref, dball_ref, dyall_ref, sem = refs[n_in:]
        n = pl.program_id(0)
        keep_dy = pltpu.make_async_copy(dy_ref, dyall_ref.at[pl.ds(slot * r, r), :], sem)

        @pl.when(n == 0)
        def _():
            keep_dy.start()

        def rows(m):
            g = dg(dy_ref[m, :], w_ref[...], NT)
            daall_ref[m, :], dball_ref[m, :] = grads(g, a_ref[m, :], b_ref[m, :])

        row_loop(r, 256, rows)

        @pl.when(n == steps - 1)
        def _():
            keep_dy.wait()

    o = spec((r, tn), lambda n, i: (0, n))
    oall = spec((r, tn), lambda n, i: (slot, n))
    return call(
        body, core, (steps,),
        [spec((r, d), lambda n, i: (0, 0), True), spec((tn, d), lambda n, i: (n, 0)), o, o] + [ANY] * (3 + len(after)),
        [(oall, (4 * r, f), bf), (oall, (4 * r, f), bf), (ANY, (4 * r, d), bf)],
        (dy, wd, a, b) + tuple(keep) + tuple(after), 2 * r * d * f,
        scratch=[pltpu.SemaphoreType.DMA], aliases={5: 0, 6: 1, 7: 2},
    )


def k_dx(core, slot, daall, dball, wg, wu, add=None, tn=512):
    f = daall.shape[1]
    r = daall.shape[0] // 4
    d = wg.shape[0]
    more = () if add is None else (add,)

    def body(i_ref, da_ref, db_ref, wg_ref, wu_ref, *rest):
        def rows(m):
            v = dg(da_ref[m, :], wg_ref[...], NT) + dg(db_ref[m, :], wu_ref[...], NT)
            rest[-1][m, :] = v if add is None else v + rest[0][m, :].astype(f32)

        row_loop(r, 256, rows)

    w = spec((tn, f), lambda n, i: (n, 0))
    hs = spec((r, f), lambda n, i: (slot(i[0]), 0), True)
    o = spec((r, tn), lambda n, i: (0, n))
    return call(
        body, core, (d // tn,), [hs, hs, w, w] + [o] * len(more),
        [(o, (r, d), f32)], (daall, dball, wg, wu) + more, 4 * r * d * f,
    )[0]


def k_dw(core, x, xo, d, do, tm=1280, tn=512):
    t, f = d.shape
    hd = x.shape[1] // 2
    nt = hd // tm

    def body(i_ref, x_ref, xo_ref, d_ref, do_ref, o_ref):
        def cols(m):
            o_ref[m, :] = dg(x_ref[:, m], d_ref[...], TN) + dg(xo_ref[:, m], do_ref[...], TN)

        row_loop(tm, 256, cols)

    xs = spec((t, tm), lambda n, m, i: (0, m + i[0] * nt))
    ds = spec((t, tn), lambda n, m, i: (0, n))
    return call(
        body, core, (pl.cdiv(f, tn), nt), [xs, xs, ds, ds],
        [(spec((tm, tn), lambda n, m, i: (m, n)), (hd, f), f32)], (x, xo, d, do), 4 * t * hd * f,
    )[0]


def k_dwd(core, h, ho, dy, dyo, tm=1152, tn=512):
    t, f = h.shape
    hd = dy.shape[1] // 2
    nt = hd // tn

    def body(i_ref, h_ref, ho_ref, d_ref, do_ref, o_ref):
        def cols(m):
            o_ref[m, :] = dg(h_ref[:, m], d_ref[...], TN) + dg(ho_ref[:, m], do_ref[...], TN)

        row_loop(tm, 384, cols)

    hs = spec((t, tm), lambda n, m, i: (0, m))
    ds = spec((t, tn), lambda n, m, i: (0, n + i[0] * nt))
    return call(
        body, core, (nt, f // tm), [hs, hs, ds, ds],
        [(spec((tm, tn), lambda n, m, i: (m, n)), (f, hd), f32)], (h, ho, dy, dyo), 4 * t * hd * f,
    )[0]


def k_add(core, u, v, sizes=None, tn=512):
    r, d = u.shape
    sizes = sizes or (r,)

    def body(i_ref, u_ref, v_ref, *outs):
        at = 0
        for size, o_ref in zip(sizes, outs):
            m = slice(at, at + size)
            o_ref[...] = u_ref[m, :] + v_ref[m, :]
            at += size

    s = spec((r, tn), lambda n, i: (0, n))
    outs = [(spec((size, tn), lambda n, i: (0, n)), (size, d), f32) for size in sizes]
    return call(body, core, (d // tn,), [s, s], outs, (u, v), r * d)


def k_fin(core, at, u, v, keep, tr):
    r, d = u.shape
    n0 = at // tr

    def body(i_ref, u_ref, v_ref, *rest):
        rest[-1][...] = (u_ref[...] + v_ref[...]).astype(bf)

    o = spec((tr, d), lambda n, i: (n0 + n, 0))
    return call(
        body, core, (v.shape[0] // tr,), [o, spec((tr, d), lambda n, i: (n, 0))] + [ANY] * len(keep),
        [(o, (r, d), bf)], (u, v) + tuple(keep), r * d, aliases={3: 0} if keep else None,
    )[0]


def solution(mesh):
    ny = mesh.shape["tp"]
    rows = P(("dp", "tp"), None)
    wsp = P("dp", "tp")
    dsp = P("tp", "dp")
    axes = ("tp", "dp")

    def hop(v, bit0, bit1):
        pairs = [(j * 2 + c, (j ^ b) * 2 + c) for j in range(ny) for c, b in enumerate((bit0, bit1))]
        return lax.ppermute(v, axes, pairs)

    def swap(v):
        return lax.ppermute(v, "dp", [(0, 1), (1, 0)])

    def layer(x, wg, wu, wd, dy):
        i = lax.axis_index("dp").astype(jnp.int32).reshape(1)
        ka = 1792
        qa = 312
        sizes = (448, 256, 48, 16)
        x1, x2 = hop(x, 1, 2), hop(x, 2, 1)
        xX, xY = jnp.where(i[0] == 0, x1, x2), jnp.where(i[0] == 0, x2, x1)
        dyX, dyY = hop(dy, 1, 1), hop(dy, 2, 2)
        wgo, wuo, wdo = swap(wg), swap(wu), swap(wd)
        wXa, wXb = hop(wd[:ka], 1, 1), hop(wd[ka:], 1, 1)
        xD = hop(xX, 2, 2)
        dyDa = hop(jnp.where(i[0] == 0, dyY[:qa], dyX[:qa]), 1, 2)
        dyDb = hop(dyX[qa:], 2, 2)
        dyD = jnp.concatenate([dyDa, dyDb], axis=0)
        wX = (wXa, wXb, swap(wXa), swap(wXb))

        a0, b0, h0, hall, xall, wgc, wuc = k_fwd0(i, x, wg, wgo, wu, wuo)
        *alls, wdc = k_g0(i, dy, wd, wdo, a0, b0)
        a1, b1, h1, hall, xall = k_fwd(i, 1, xX, wgc, wuc, hall, xall)
        a2, b2, h2, hall, xall = k_fwd(i, 2, xY, wgc, wuc, hall, xall)
        a3, b3, h3, hall, xall = k_fwd(i, 3, xD, wgc, wuc, hall, xall)

        alls = k_g(i, 1, dyX, wdc, a1, b1, alls)
        alls = k_g(i, 2, dyY, wdc, a2, b2, alls)
        z1 = k_dx(i, lambda c: 1 + c, alls[0], alls[1], wgc, wuc)
        s1 = hop(z1, 1, 2)
        z0 = k_dx(i, lambda c: 0, alls[0], alls[1], wgc, wuc, add=dy)
        daall, dball, dyall = k_g(i, 3, dyD, wdc, a3, b3, alls, (z0, z1))
        z3 = k_dx(i, lambda c: 3, daall, dball, wgc, wuc)
        sa = hop(z3, 1, 2)
        z2 = k_dx(i, lambda c: 2 - c, daall, dball, wgc, wuc)
        s2 = k_add(i, z2, sa, sizes)
        s2 = [hop(v, 2, 1) for v in s2]

        hDr, hXr = hop(h3, 1, 1), hop(h1, 1, 1)
        yYr = hop(k_y2(i, h2, wdc, hDr, wX), 2, 2)
        y = k_y2(i, h0, wdc, hXr, wX, (x, yYr))

        xallo, hallo = swap(xall), swap(hall)
        dyallo, daallo, dballo = swap(dyall), swap(daall), swap(dball)
        dwd = k_dwd(i, hall, hallo, dyall, dyallo)
        dwg = k_dw(i, xall, xallo, daall, daallo)
        dwu = k_dw(i, xall, xallo, dball, dballo)

        pre = k_add(i, z0, s1)[0]
        dx = ()
        for p, v in enumerate(s2):
            dx = (k_fin(i, sum(sizes[:p]), pre, v, dx, 64 if p < 2 else 16),)
        return y, dx[0], dwg, dwu, dwd

    return jax.shard_map(layer, mesh=mesh, in_specs=(rows, wsp, wsp, dsp, rows), out_specs=(rows, rows, wsp, wsp, dsp), check_vma=False)
```

```python
import jax
import jax.numpy as jnp
from jax import lax
from jax.experimental import pallas as pl
from jax.experimental.pallas import tpu as pltpu
from jax.sharding import PartitionSpec as P


f32 = jnp.float32
bf = jnp.bfloat16
NT = (((1,), (1,)), ((), ()))
TN = (((0,), (0,)), ((), ()))
VMEM = 62 * 1024 * 1024
ONE = pl.Buffered(1)
ANY = pl.BlockSpec(memory_space=pl.ANY)


def mm(u, v):
    return jnp.dot(u, v, preferred_element_type=f32)


def dg(u, v, dims):
    return lax.dot_general(u, v, dims, preferred_element_type=f32)


def sds(shape, dtype):
    return jax.ShapeDtypeStruct(shape, dtype)


def spec(shape, index, once=False):
    if once:
        return pl.BlockSpec(shape, index, pipeline_mode=ONE)
    return pl.BlockSpec(shape, index)


def row_loop(rows, step, fn):
    def trip(m, carry):
        fn(pl.ds(pl.multiple_of(m * step, step), step))
        return carry

    lax.fori_loop(0, rows // step, trip, 0)


def call(body, core, grid, ins, outs, args, flops, scratch=(), aliases=None):
    moved = sum(a.size * a.dtype.itemsize for a in args)
    return pl.pallas_call(
        body,
        grid_spec=pltpu.PrefetchScalarGridSpec(
            num_scalar_prefetch=1, grid=grid, in_specs=list(ins), out_specs=[o[0] for o in outs], scratch_shapes=list(scratch)
        ),
        out_shape=[sds(o[1], o[2]) for o in outs],
        input_output_aliases=aliases or {},
        compiler_params=pltpu.CompilerParams(dimension_semantics=("arbitrary",) * len(grid), vmem_limit_bytes=VMEM),
        cost_estimate=pl.CostEstimate(flops=int(flops), bytes_accessed=int(moved), transcendentals=0),
    )(core, *args)


def silu_h(a, b):
    return (a * jax.nn.sigmoid(a) * b).astype(bf)


def k_fwd0(core, x, wg, wgo, wu, wuo, tn=512):
    r, d = x.shape
    hd, f = wg.shape
    steps = pl.cdiv(f, tn)
    last = f - (steps - 1) * tn

    def body(i_ref, x_ref, wg_ref, wgo_ref, wu_ref, wuo_ref, a_ref, b_ref, h_ref, hall_ref, xall_ref, wgc_ref, wuc_ref, sem, wsem):
        n = pl.program_id(0)
        s = pl.multiple_of(i_ref[0] * hd, 128)
        o = pl.multiple_of((1 - i_ref[0]) * hd, 128)
        keep_x = pltpu.make_async_copy(x_ref, xall_ref.at[pl.ds(0, r), :], sem)

        def copies(width):
            c = pl.ds(pl.multiple_of(n * tn, 128), width)
            moves = ((wg_ref, wgc_ref, s), (wgo_ref, wgc_ref, o), (wu_ref, wuc_ref, s), (wuo_ref, wuc_ref, o))
            return [
                pltpu.make_async_copy(u.at[:, pl.ds(0, width)], v.at[pl.ds(q, hd), c], wsem.at[k])
                for k, (u, v, q) in enumerate(moves)
            ]

        @pl.when(n == 0)
        def _():
            keep_x.start()

        @pl.when(n < steps - 1)
        def _():
            for c in copies(tn):
                c.start()

        @pl.when(n == steps - 1)
        def _():
            for c in copies(last):
                c.start()

        def rows(m):
            xs = x_ref[m, pl.ds(s, hd)]
            xo = x_ref[m, pl.ds(o, hd)]
            a = mm(xs, wg_ref[...]) + mm(xo, wgo_ref[...])
            b = mm(xs, wu_ref[...]) + mm(xo, wuo_ref[...])
            a_ref[m, :] = a
            b_ref[m, :] = b
            h = silu_h(a, b)
            h_ref[m, :] = h
            hall_ref[m, :] = h

        row_loop(r, 256, rows)

        @pl.when(n < steps - 1)
        def _():
            for c in copies(tn):
                c.wait()

        @pl.when(n == steps - 1)
        def _():
            for c in copies(last):
                c.wait()
            keep_x.wait()

    w = spec((hd, tn), lambda n, i: (0, n))
    o = spec((r, tn), lambda n, i: (0, n))
    return call(
        body, core, (steps,),
        [spec((r, d), lambda n, i: (0, 0), True), w, w, w, w],
        [(o, (r, f), f32), (o, (r, f), f32), (o, (r, f), bf), (o, (4 * r, f), bf), (ANY, (4 * r, d), bf),
         (ANY, (d, f), bf), (ANY, (d, f), bf)],
        (x, wg, wgo, wu, wuo), 4 * r * d * f,
        scratch=[pltpu.SemaphoreType.DMA, pltpu.SemaphoreType.DMA((4,))],
    )


def k_fwd(core, slot, x, wg, wu, hall, xall, tn=512):
    r, d = x.shape
    f = wg.shape[1]
    steps = pl.cdiv(f, tn)

    def body(i_ref, x_ref, wg_ref, wu_ref, hin_ref, xin_ref, a_ref, b_ref, h_ref, hall_ref, xall_ref, sem):
        n = pl.program_id(0)
        keep_x = pltpu.make_async_copy(x_ref, xall_ref.at[pl.ds(slot * r, r), :], sem)

        @pl.when(n == 0)
        def _():
            keep_x.start()

        def rows(m):
            a = mm(x_ref[m, :], wg_ref[...])
            b = mm(x_ref[m, :], wu_ref[...])
            a_ref[m, :] = a
            b_ref[m, :] = b
            h = silu_h(a, b)
            h_ref[m, :] = h
            hall_ref[m, :] = h

        row_loop(r, 256, rows)

        @pl.when(n == steps - 1)
        def _():
            keep_x.wait()

    w = spec((d, tn), lambda n, i: (0, n))
    o = spec((r, tn), lambda n, i: (0, n))
    return call(
        body, core, (steps,),
        [spec((r, d), lambda n, i: (0, 0), True), w, w, ANY, ANY],
        [(o, (r, f), f32), (o, (r, f), f32), (o, (r, f), bf),
         (spec((r, tn), lambda n, i: (slot, n)), (4 * r, f), bf), (ANY, (4 * r, d), bf)],
        (x, wg, wu, hall, xall), 4 * r * d * f,
        scratch=[pltpu.SemaphoreType.DMA], aliases={4: 3, 5: 4},
    )


def k_y2(core, h, wd, hr, ws, res=None, tn=512):
    r, f = h.shape
    d = wd.shape[1]
    ka = ws[0].shape[0]
    nt = d // 2 // tn

    def body(i_ref, h_ref, w_ref, hr_ref, *rest):
        n = pl.program_id(0)
        own = (n < nt) == (i_ref[0] == 0)
        o_ref = rest[-1]

        def part(ua, ub):
            def rows(m):
                v = mm(h_ref[m, :], w_ref[...]) + (mm(hr_ref[m, :ka], ua[...]) + mm(hr_ref[m, ka:], ub[...]))
                if res is not None:
                    v = (rest[4][m, :].astype(f32) + v + rest[5][m, :]).astype(bf)
                o_ref[m, :] = v

            row_loop(r, 256, rows)

        @pl.when(own)
        def _():
            part(rest[0], rest[1])

        @pl.when(jnp.logical_not(own))
        def _():
            part(rest[2], rest[3])

    o = spec((r, tn), lambda n, i: (0, n))
    hs = spec((r, f), lambda n, i: (0, 0), True)

    def part_spec(k, other):
        return spec((k, tn), lambda n, i: (0, jnp.clip(n - ((1 - i[0]) if other else i[0]) * nt, 0, nt - 1)))

    more = () if res is None else tuple(res)
    return call(
        body, core, (2 * nt,),
        [hs, spec((f, tn), lambda n, i: (0, n)), hs]
        + [part_spec(ka, False), part_spec(f - ka, False), part_spec(ka, True), part_spec(f - ka, True)] + [o] * len(more),
        [(o, (r, d), f32 if res is None else bf)], (h, wd, hr) + tuple(ws) + more, 4 * r * d * f,
    )[0]


def grads(g, a, b):
    sig = jax.nn.sigmoid(a)
    return (g * b * sig * (1.0 + a * (1.0 - sig))).astype(bf), (g * (a * sig)).astype(bf)


def k_g0(core, dy, wd, wdo, a, b, tn=512):
    r, d = dy.shape
    f, hd = wd.shape
    steps = pl.cdiv(f, tn)
    last = f - (steps - 1) * tn

    def body(i_ref, dy_ref, w_ref, wo_ref, a_ref, b_ref, daall_ref, dball_ref, dyall_ref, wc_ref, sem, wsem):
        n = pl.program_id(0)
        s = pl.multiple_of(i_ref[0] * hd, 128)
        o = pl.multiple_of((1 - i_ref[0]) * hd, 128)
        keep_dy = pltpu.make_async_copy(dy_ref, dyall_ref.at[pl.ds(0, r), :], sem)

        def copies(height):
            c = pl.ds(pl.multiple_of(n * tn, 128), height)
            return [
                pltpu.make_async_copy(u.at[pl.ds(0, height), :], wc_ref.at[c, pl.ds(q, hd)], wsem.at[k])
                for k, (u, q) in enumerate(((w_ref, s), (wo_ref, o)))
            ]

        @pl.when(n == 0)
        def _():
            keep_dy.start()

        @pl.when(n < steps - 1)
        def _():
            for c in copies(tn):
                c.start()

        @pl.when(n == steps - 1)
        def _():
            for c in copies(last):
                c.start()

        def rows(m):
            g = dg(dy_ref[m, pl.ds(s, hd)], w_ref[...], NT) + dg(dy_ref[m, pl.ds(o, hd)], wo_ref[...], NT)
            daall_ref[m, :], dball_ref[m, :] = grads(g, a_ref[m, :], b_ref[m, :])

        row_loop(r, 256, rows)

        @pl.when(n < steps - 1)
        def _():
            for c in copies(tn):
                c.wait()

        @pl.when(n == steps - 1)
        def _():
            for c in copies(last):
                c.wait()
            keep_dy.wait()

    o = spec((r, tn), lambda n, i: (0, n))
    w = spec((tn, hd), lambda n, i: (n, 0))
    return call(
        body, core, (steps,),
        [spec((r, d), lambda n, i: (0, 0), True), w, w, o, o],
        [(o, (4 * r, f), bf), (o, (4 * r, f), bf), (ANY, (4 * r, d), bf), (ANY, (f, d), bf)],
        (dy, wd, wdo, a, b), 2 * r * d * f,
        scratch=[pltpu.SemaphoreType.DMA, pltpu.SemaphoreType.DMA((2,))],
    )


def k_g(core, slot, dy, wd, a, b, keep, after=(), tn=512):
    r, d = dy.shape
    f = wd.shape[0]
    steps = pl.cdiv(f, tn)
    n_in = 8 + len(after)

    def body(*refs):
        _, dy_ref, w_ref, a_ref, b_ref = refs[:5]
        daall_ref, dball_ref, dyall_ref, sem = refs[n_in:]
        n = pl.program_id(0)
        keep_dy = pltpu.make_async_copy(dy_ref, dyall_ref.at[pl.ds(slot * r, r), :], sem)

        @pl.when(n == 0)
        def _():
            keep_dy.start()

        def rows(m):
            g = dg(dy_ref[m, :], w_ref[...], NT)
            daall_ref[m, :], dball_ref[m, :] = grads(g, a_ref[m, :], b_ref[m, :])

        row_loop(r, 256, rows)

        @pl.when(n == steps - 1)
        def _():
            keep_dy.wait()

    o = spec((r, tn), lambda n, i: (0, n))
    oall = spec((r, tn), lambda n, i: (slot, n))
    return call(
        body, core, (steps,),
        [spec((r, d), lambda n, i: (0, 0), True), spec((tn, d), lambda n, i: (n, 0)), o, o] + [ANY] * (3 + len(after)),
        [(oall, (4 * r, f), bf), (oall, (4 * r, f), bf), (ANY, (4 * r, d), bf)],
        (dy, wd, a, b) + tuple(keep) + tuple(after), 2 * r * d * f,
        scratch=[pltpu.SemaphoreType.DMA], aliases={5: 0, 6: 1, 7: 2},
    )


def k_dx(core, slot, daall, dball, wg, wu, add=None, tn=512):
    f = daall.shape[1]
    r = daall.shape[0] // 4
    d = wg.shape[0]
    more = () if add is None else (add,)

    def body(i_ref, da_ref, db_ref, wg_ref, wu_ref, *rest):
        def rows(m):
            v = dg(da_ref[m, :], wg_ref[...], NT) + dg(db_ref[m, :], wu_ref[...], NT)
            rest[-1][m, :] = v if add is None else v + rest[0][m, :].astype(f32)

        row_loop(r, 256, rows)

    w = spec((tn, f), lambda n, i: (n, 0))
    hs = spec((r, f), lambda n, i: (slot(i[0]), 0), True)
    o = spec((r, tn), lambda n, i: (0, n))
    return call(
        body, core, (d // tn,), [hs, hs, w, w] + [o] * len(more),
        [(o, (r, d), f32)], (daall, dball, wg, wu) + more, 4 * r * d * f,
    )[0]


def k_dw(core, x, xo, d, do, tm=1280, tn=512):
    t, f = d.shape
    hd = x.shape[1] // 2
    nt = hd // tm

    def body(i_ref, x_ref, xo_ref, d_ref, do_ref, o_ref):
        def cols(m):
            o_ref[m, :] = dg(x_ref[:, m], d_ref[...], TN) + dg(xo_ref[:, m], do_ref[...], TN)

        row_loop(tm, 256, cols)

    xs = spec((t, tm), lambda n, m, i: (0, m + i[0] * nt))
    ds = spec((t, tn), lambda n, m, i: (0, n))
    return call(
        body, core, (pl.cdiv(f, tn), nt), [xs, xs, ds, ds],
        [(spec((tm, tn), lambda n, m, i: (m, n)), (hd, f), f32)], (x, xo, d, do), 4 * t * hd * f,
    )[0]


def k_dwd(core, h, ho, dy, dyo, tm=1152, tn=512):
    t, f = h.shape
    hd = dy.shape[1] // 2
    nt = hd // tn

    def body(i_ref, h_ref, ho_ref, d_ref, do_ref, o_ref):
        def cols(m):
            o_ref[m, :] = dg(h_ref[:, m], d_ref[...], TN) + dg(ho_ref[:, m], do_ref[...], TN)

        row_loop(tm, 384, cols)

    hs = spec((t, tm), lambda n, m, i: (0, m))
    ds = spec((t, tn), lambda n, m, i: (0, n + i[0] * nt))
    return call(
        body, core, (nt, f // tm), [hs, hs, ds, ds],
        [(spec((tm, tn), lambda n, m, i: (m, n)), (f, hd), f32)], (h, ho, dy, dyo), 4 * t * hd * f,
    )[0]


def k_add(core, u, v, sizes=None, tn=512):
    r, d = u.shape
    sizes = sizes or (r,)

    def body(i_ref, u_ref, v_ref, *outs):
        at = 0
        for size, o_ref in zip(sizes, outs):
            m = slice(at, at + size)
            o_ref[...] = u_ref[m, :] + v_ref[m, :]
            at += size

    s = spec((r, tn), lambda n, i: (0, n))
    outs = [(spec((size, tn), lambda n, i: (0, n)), (size, d), f32) for size in sizes]
    return call(body, core, (d // tn,), [s, s], outs, (u, v), r * d)


def k_fin(core, at, u, v, keep, tr):
    r, d = u.shape
    n0 = at // tr

    def body(i_ref, u_ref, v_ref, *rest):
        rest[-1][...] = (u_ref[...] + v_ref[...]).astype(bf)

    o = spec((tr, d), lambda n, i: (n0 + n, 0))
    return call(
        body, core, (v.shape[0] // tr,), [o, spec((tr, d), lambda n, i: (n, 0))] + [ANY] * len(keep),
        [(o, (r, d), bf)], (u, v) + tuple(keep), r * d, aliases={3: 0} if keep else None,
    )[0]


def solution(mesh):
    ny = mesh.shape["tp"]
    rows = P(("dp", "tp"), None)
    wsp = P("dp", "tp")
    dsp = P("tp", "dp")
    axes = ("tp", "dp")

    def hop(v, bit0, bit1):
        pairs = [(j * 2 + c, (j ^ b) * 2 + c) for j in range(ny) for c, b in enumerate((bit0, bit1))]
        return lax.ppermute(v, axes, pairs)

    def swap(v):
        return lax.ppermute(v, "dp", [(0, 1), (1, 0)])

    def layer(x, wg, wu, wd, dy):
        i = lax.axis_index("dp").astype(jnp.int32).reshape(1)
        ka = 1792
        qa = 304
        sizes = (432, 288, 32, 16)
        x1, x2 = hop(x, 1, 2), hop(x, 2, 1)
        xX, xY = jnp.where(i[0] == 0, x1, x2), jnp.where(i[0] == 0, x2, x1)
        dyX, dyY = hop(dy, 1, 1), hop(dy, 2, 2)
        wgo, wuo, wdo = swap(wg), swap(wu), swap(wd)
        wXa, wXb = hop(wd[:ka], 1, 1), hop(wd[ka:], 1, 1)
        xD = hop(xX, 2, 2)
        qb = qa + 8
        hd = wg.shape[0]
        part = jnp.where(i[0] == 0, dyY[:qb], dyX[:qb])
        dyDa = hop(part[:qa], 1, 2)
        dyDc = hop(part[qa:, :hd], 1, 2)
        dyDe = hop(dyX[qa:qb, hd:], 2, 2)
        dyDb = hop(dyX[qb:], 2, 2)
        dyD = jnp.concatenate([dyDa, jnp.concatenate([dyDc, dyDe], axis=1), dyDb], axis=0)
        wX = (wXa, wXb, swap(wXa), swap(wXb))

        a0, b0, h0, hall, xall, wgc, wuc = k_fwd0(i, x, wg, wgo, wu, wuo)
        *alls, wdc = k_g0(i, dy, wd, wdo, a0, b0)
        a1, b1, h1, hall, xall = k_fwd(i, 1, xX, wgc, wuc, hall, xall)
        a2, b2, h2, hall, xall = k_fwd(i, 2, xY, wgc, wuc, hall, xall)
        a3, b3, h3, hall, xall = k_fwd(i, 3, xD, wgc, wuc, hall, xall)

        alls = k_g(i, 1, dyX, wdc, a1, b1, alls)
        alls = k_g(i, 2, dyY, wdc, a2, b2, alls)
        z1 = k_dx(i, lambda c: 1 + c, alls[0], alls[1], wgc, wuc)
        s1 = hop(z1, 1, 2)
        z0 = k_dx(i, lambda c: 0, alls[0], alls[1], wgc, wuc, add=dy)
        daall, dball, dyall = k_g(i, 3, dyD, wdc, a3, b3, alls, (z0, z1))
        z3 = k_dx(i, lambda c: 3, daall, dball, wgc, wuc)
        sa = hop(z3, 1, 2)
        z2 = k_dx(i, lambda c: 2 - c, daall, dball, wgc, wuc)
        s2 = k_add(i, z2, sa, sizes)
        s2 = [hop(v, 2, 1) for v in s2]

        hDr, hXr = hop(h3, 1, 1), hop(h1, 1, 1)
        yYr = hop(k_y2(i, h2, wdc, hDr, wX), 2, 2)
        y = k_y2(i, h0, wdc, hXr, wX, (x, yYr))

        xallo, hallo = swap(xall), swap(hall)
        dyallo, daallo, dballo = swap(dyall), swap(daall), swap(dball)
        dwd = k_dwd(i, hall, hallo, dyall, dyallo)
        dwg = k_dw(i, xall, xallo, daall, daallo)
        dwu = k_dw(i, xall, xallo, dball, dballo)

        pre = k_add(i, z0, s1)[0]
        dx = ()
        for p, v in enumerate(s2):
            dx = (k_fin(i, sum(sizes[:p]), pre, v, dx, 48 if p < 2 else 16),)
        return y, dx[0], dwg, dwu, dwd

    return jax.shard_map(layer, mesh=mesh, in_specs=(rows, wsp, wsp, dsp, rows), out_specs=(rows, rows, wsp, wsp, dsp), check_vma=False)
```

```python
import jax
import jax.numpy as jnp
from jax import lax
from jax.experimental import pallas as pl
from jax.experimental.pallas import tpu as pltpu
from jax.sharding import PartitionSpec as P


f32 = jnp.float32
bf = jnp.bfloat16
NT = (((1,), (1,)), ((), ()))
TN = (((0,), (0,)), ((), ()))
VMEM = 62 * 1024 * 1024
ONE = pl.Buffered(1)
ANY = pl.BlockSpec(memory_space=pl.ANY)


def mm(u, v):
    return jnp.dot(u, v, preferred_element_type=f32)


def dg(u, v, dims):
    return lax.dot_general(u, v, dims, preferred_element_type=f32)


def sds(shape, dtype):
    return jax.ShapeDtypeStruct(shape, dtype)


def spec(shape, index, once=False):
    if once:
        return pl.BlockSpec(shape, index, pipeline_mode=ONE)
    return pl.BlockSpec(shape, index)


def row_loop(rows, step, fn):
    def trip(m, carry):
        fn(pl.ds(pl.multiple_of(m * step, step), step))
        return carry

    lax.fori_loop(0, rows // step, trip, 0)


def call(body, core, grid, ins, outs, args, flops, scratch=(), aliases=None):
    moved = sum(a.size * a.dtype.itemsize for a in args)
    return pl.pallas_call(
        body,
        grid_spec=pltpu.PrefetchScalarGridSpec(
            num_scalar_prefetch=1, grid=grid, in_specs=list(ins), out_specs=[o[0] for o in outs], scratch_shapes=list(scratch)
        ),
        out_shape=[sds(o[1], o[2]) for o in outs],
        input_output_aliases=aliases or {},
        compiler_params=pltpu.CompilerParams(dimension_semantics=("arbitrary",) * len(grid), vmem_limit_bytes=VMEM),
        cost_estimate=pl.CostEstimate(flops=int(flops), bytes_accessed=int(moved), transcendentals=0),
    )(core, *args)


def silu_h(a, b):
    return (a * jax.nn.sigmoid(a) * b).astype(bf)


def k_fwd0(core, x, wg, wgo, wu, wuo, tn=512):
    r, d = x.shape
    hd, f = wg.shape
    steps = pl.cdiv(f, tn)
    last = f - (steps - 1) * tn

    def body(i_ref, x_ref, wg_ref, wgo_ref, wu_ref, wuo_ref, a_ref, b_ref, h_ref, hall_ref, xall_ref, wgc_ref, wuc_ref, sem, wsem):
        n = pl.program_id(0)
        s = pl.multiple_of(i_ref[0] * hd, 128)
        o = pl.multiple_of((1 - i_ref[0]) * hd, 128)
        keep_x = pltpu.make_async_copy(x_ref, xall_ref.at[pl.ds(0, r), :], sem)

        def copies(width):
            c = pl.ds(pl.multiple_of(n * tn, 128), width)
            moves = ((wg_ref, wgc_ref, s), (wgo_ref, wgc_ref, o), (wu_ref, wuc_ref, s), (wuo_ref, wuc_ref, o))
            return [
                pltpu.make_async_copy(u.at[:, pl.ds(0, width)], v.at[pl.ds(q, hd), c], wsem.at[k])
                for k, (u, v, q) in enumerate(moves)
            ]

        @pl.when(n == 0)
        def _():
            keep_x.start()

        @pl.when(n < steps - 1)
        def _():
            for c in copies(tn):
                c.start()

        @pl.when(n == steps - 1)
        def _():
            for c in copies(last):
                c.start()

        def rows(m):
            xs = x_ref[m, pl.ds(s, hd)]
            xo = x_ref[m, pl.ds(o, hd)]
            a = mm(xs, wg_ref[...]) + mm(xo, wgo_ref[...])
            b = mm(xs, wu_ref[...]) + mm(xo, wuo_ref[...])
            a_ref[m, :] = a
            b_ref[m, :] = b
            h = silu_h(a, b)
            h_ref[m, :] = h
            hall_ref[m, :] = h

        row_loop(r, 256, rows)

        @pl.when(n < steps - 1)
        def _():
            for c in copies(tn):
                c.wait()

        @pl.when(n == steps - 1)
        def _():
            for c in copies(last):
                c.wait()
            keep_x.wait()

    w = spec((hd, tn), lambda n, i: (0, n))
    o = spec((r, tn), lambda n, i: (0, n))
    return call(
        body, core, (steps,),
        [spec((r, d), lambda n, i: (0, 0), True), w, w, w, w],
        [(o, (r, f), f32), (o, (r, f), f32), (o, (r, f), bf), (o, (4 * r, f), bf), (ANY, (4 * r, d), bf),
         (ANY, (d, f), bf), (ANY, (d, f), bf)],
        (x, wg, wgo, wu, wuo), 4 * r * d * f,
        scratch=[pltpu.SemaphoreType.DMA, pltpu.SemaphoreType.DMA((4,))],
    )


def k_fwd(core, slot, x, wg, wu, hall, xall, tn=512):
    r, d = x.shape
    f = wg.shape[1]
    steps = pl.cdiv(f, tn)

    def body(i_ref, x_ref, wg_ref, wu_ref, hin_ref, xin_ref, a_ref, b_ref, h_ref, hall_ref, xall_ref, sem):
        n = pl.program_id(0)
        keep_x = pltpu.make_async_copy(x_ref, xall_ref.at[pl.ds(slot * r, r), :], sem)

        @pl.when(n == 0)
        def _():
            keep_x.start()

        def rows(m):
            a = mm(x_ref[m, :], wg_ref[...])
            b = mm(x_ref[m, :], wu_ref[...])
            a_ref[m, :] = a
            b_ref[m, :] = b
            h = silu_h(a, b)
            h_ref[m, :] = h
            hall_ref[m, :] = h

        row_loop(r, 256, rows)

        @pl.when(n == steps - 1)
        def _():
            keep_x.wait()

    w = spec((d, tn), lambda n, i: (0, n))
    o = spec((r, tn), lambda n, i: (0, n))
    return call(
        body, core, (steps,),
        [spec((r, d), lambda n, i: (0, 0), True), w, w, ANY, ANY],
        [(o, (r, f), f32), (o, (r, f), f32), (o, (r, f), bf),
         (spec((r, tn), lambda n, i: (slot, n)), (4 * r, f), bf), (ANY, (4 * r, d), bf)],
        (x, wg, wu, hall, xall), 4 * r * d * f,
        scratch=[pltpu.SemaphoreType.DMA], aliases={4: 3, 5: 4},
    )


def k_y2(core, h, wd, hr, ws, res=None, tn=512):
    r, f = h.shape
    d = wd.shape[1]
    ka = ws[0].shape[0]
    nt = d // 2 // tn

    def body(i_ref, h_ref, w_ref, hr_ref, *rest):
        n = pl.program_id(0)
        own = (n < nt) == (i_ref[0] == 0)
        o_ref = rest[-1]

        def part(ua, ub):
            def rows(m):
                v = mm(h_ref[m, :], w_ref[...]) + (mm(hr_ref[m, :ka], ua[...]) + mm(hr_ref[m, ka:], ub[...]))
                if res is not None:
                    v = (rest[4][m, :].astype(f32) + v + rest[5][m, :]).astype(bf)
                o_ref[m, :] = v

            row_loop(r, 256, rows)

        @pl.when(own)
        def _():
            part(rest[0], rest[1])

        @pl.when(jnp.logical_not(own))
        def _():
            part(rest[2], rest[3])

    o = spec((r, tn), lambda n, i: (0, n))
    hs = spec((r, f), lambda n, i: (0, 0), True)

    def part_spec(k, other):
        return spec((k, tn), lambda n, i: (0, jnp.clip(n - ((1 - i[0]) if other else i[0]) * nt, 0, nt - 1)))

    more = () if res is None else tuple(res)
    return call(
        body, core, (2 * nt,),
        [hs, spec((f, tn), lambda n, i: (0, n)), hs]
        + [part_spec(ka, False), part_spec(f - ka, False), part_spec(ka, True), part_spec(f - ka, True)] + [o] * len(more),
        [(o, (r, d), f32 if res is None else bf)], (h, wd, hr) + tuple(ws) + more, 4 * r * d * f,
    )[0]


def grads(g, a, b):
    sig = jax.nn.sigmoid(a)
    return (g * b * sig * (1.0 + a * (1.0 - sig))).astype(bf), (g * (a * sig)).astype(bf)


def k_g0(core, dy, wd, wdo, a, b, tn=512):
    r, d = dy.shape
    f, hd = wd.shape
    steps = pl.cdiv(f, tn)
    last = f - (steps - 1) * tn

    def body(i_ref, dy_ref, w_ref, wo_ref, a_ref, b_ref, daall_ref, dball_ref, dyall_ref, wc_ref, sem, wsem):
        n = pl.program_id(0)
        s = pl.multiple_of(i_ref[0] * hd, 128)
        o = pl.multiple_of((1 - i_ref[0]) * hd, 128)
        keep_dy = pltpu.make_async_copy(dy_ref, dyall_ref.at[pl.ds(0, r), :], sem)

        def copies(height):
            c = pl.ds(pl.multiple_of(n * tn, 128), height)
            return [
                pltpu.make_async_copy(u.at[pl.ds(0, height), :], wc_ref.at[c, pl.ds(q, hd)], wsem.at[k])
                for k, (u, q) in enumerate(((w_ref, s), (wo_ref, o)))
            ]

        @pl.when(n == 0)
        def _():
            keep_dy.start()

        @pl.when(n < steps - 1)
        def _():
            for c in copies(tn):
                c.start()

        @pl.when(n == steps - 1)
        def _():
            for c in copies(last):
                c.start()

        def rows(m):
            g = dg(dy_ref[m, pl.ds(s, hd)], w_ref[...], NT) + dg(dy_ref[m, pl.ds(o, hd)], wo_ref[...], NT)
            daall_ref[m, :], dball_ref[m, :] = grads(g, a_ref[m, :], b_ref[m, :])

        row_loop(r, 256, rows)

        @pl.when(n < steps - 1)
        def _():
            for c in copies(tn):
                c.wait()

        @pl.when(n == steps - 1)
        def _():
            for c in copies(last):
                c.wait()
            keep_dy.wait()

    o = spec((r, tn), lambda n, i: (0, n))
    w = spec((tn, hd), lambda n, i: (n, 0))
    return call(
        body, core, (steps,),
        [spec((r, d), lambda n, i: (0, 0), True), w, w, o, o],
        [(o, (4 * r, f), bf), (o, (4 * r, f), bf), (ANY, (4 * r, d), bf), (ANY, (f, d), bf)],
        (dy, wd, wdo, a, b), 2 * r * d * f,
        scratch=[pltpu.SemaphoreType.DMA, pltpu.SemaphoreType.DMA((2,))],
    )


def k_g(core, slot, dy, wd, a, b, keep, after=(), tn=512):
    r, d = dy.shape
    f = wd.shape[0]
    steps = pl.cdiv(f, tn)
    n_in = 8 + len(after)

    def body(*refs):
        _, dy_ref, w_ref, a_ref, b_ref = refs[:5]
        daall_ref, dball_ref, dyall_ref, sem = refs[n_in:]
        n = pl.program_id(0)
        keep_dy = pltpu.make_async_copy(dy_ref, dyall_ref.at[pl.ds(slot * r, r), :], sem)

        @pl.when(n == 0)
        def _():
            keep_dy.start()

        def rows(m):
            g = dg(dy_ref[m, :], w_ref[...], NT)
            daall_ref[m, :], dball_ref[m, :] = grads(g, a_ref[m, :], b_ref[m, :])

        row_loop(r, 256, rows)

        @pl.when(n == steps - 1)
        def _():
            keep_dy.wait()

    o = spec((r, tn), lambda n, i: (0, n))
    oall = spec((r, tn), lambda n, i: (slot, n))
    return call(
        body, core, (steps,),
        [spec((r, d), lambda n, i: (0, 0), True), spec((tn, d), lambda n, i: (n, 0)), o, o] + [ANY] * (3 + len(after)),
        [(oall, (4 * r, f), bf), (oall, (4 * r, f), bf), (ANY, (4 * r, d), bf)],
        (dy, wd, a, b) + tuple(keep) + tuple(after), 2 * r * d * f,
        scratch=[pltpu.SemaphoreType.DMA], aliases={5: 0, 6: 1, 7: 2},
    )


def k_dx(core, slot, daall, dball, wg, wu, add=None, tn=512):
    f = daall.shape[1]
    r = daall.shape[0] // 4
    d = wg.shape[0]
    more = () if add is None else (add,)

    def body(i_ref, da_ref, db_ref, wg_ref, wu_ref, *rest):
        def rows(m):
            v = dg(da_ref[m, :], wg_ref[...], NT) + dg(db_ref[m, :], wu_ref[...], NT)
            rest[-1][m, :] = v if add is None else v + rest[0][m, :].astype(f32)

        row_loop(r, 256, rows)

    w = spec((tn, f), lambda n, i: (n, 0))
    hs = spec((r, f), lambda n, i: (slot(i[0]), 0), True)
    o = spec((r, tn), lambda n, i: (0, n))
    return call(
        body, core, (d // tn,), [hs, hs, w, w] + [o] * len(more),
        [(o, (r, d), f32)], (daall, dball, wg, wu) + more, 4 * r * d * f,
    )[0]


def k_dw(core, x, xo, d, do, tm=1280, tn=512):
    t, f = d.shape
    hd = x.shape[1] // 2
    nt = hd // tm

    def body(i_ref, x_ref, xo_ref, d_ref, do_ref, o_ref):
        def cols(m):
            o_ref[m, :] = dg(x_ref[:, m], d_ref[...], TN) + dg(xo_ref[:, m], do_ref[...], TN)

        row_loop(tm, 256, cols)

    xs = spec((t, tm), lambda n, m, i: (0, m + i[0] * nt))
    ds = spec((t, tn), lambda n, m, i: (0, n))
    return call(
        body, core, (pl.cdiv(f, tn), nt), [xs, xs, ds, ds],
        [(spec((tm, tn), lambda n, m, i: (m, n)), (hd, f), f32)], (x, xo, d, do), 4 * t * hd * f,
    )[0]


def k_dwd(core, h, ho, dy, dyo, tm=1152, tn=512):
    t, f = h.shape
    hd = dy.shape[1] // 2
    nt = hd // tn

    def body(i_ref, h_ref, ho_ref, d_ref, do_ref, o_ref):
        def cols(m):
            o_ref[m, :] = dg(h_ref[:, m], d_ref[...], TN) + dg(ho_ref[:, m], do_ref[...], TN)

        row_loop(tm, 384, cols)

    hs = spec((t, tm), lambda n, m, i: (0, m))
    ds = spec((t, tn), lambda n, m, i: (0, n + i[0] * nt))
    return call(
        body, core, (nt, f // tm), [hs, hs, ds, ds],
        [(spec((tm, tn), lambda n, m, i: (m, n)), (f, hd), f32)], (h, ho, dy, dyo), 4 * t * hd * f,
    )[0]


def k_add(core, u, v, sizes=None, tn=512):
    r, d = u.shape
    sizes = sizes or (r,)

    def body(i_ref, u_ref, v_ref, *outs):
        at = 0
        for size, o_ref in zip(sizes, outs):
            m = slice(at, at + size)
            o_ref[...] = u_ref[m, :] + v_ref[m, :]
            at += size

    s = spec((r, tn), lambda n, i: (0, n))
    outs = [(spec((size, tn), lambda n, i: (0, n)), (size, d), f32) for size in sizes]
    return call(body, core, (d // tn,), [s, s], outs, (u, v), r * d)


def k_fin(core, at, u, v, keep, tr):
    r, d = u.shape
    n0 = at // tr

    def body(i_ref, u_ref, v_ref, *rest):
        rest[-1][...] = (u_ref[...] + v_ref[...]).astype(bf)

    o = spec((tr, d), lambda n, i: (n0 + n, 0))
    return call(
        body, core, (v.shape[0] // tr,), [o, spec((tr, d), lambda n, i: (n, 0))] + [ANY] * len(keep),
        [(o, (r, d), bf)], (u, v) + tuple(keep), r * d, aliases={3: 0} if keep else None,
    )[0]


def solution(mesh):
    ny = mesh.shape["tp"]
    rows = P(("dp", "tp"), None)
    wsp = P("dp", "tp")
    dsp = P("tp", "dp")
    axes = ("tp", "dp")

    def hop(v, bit0, bit1):
        pairs = [(j * 2 + c, (j ^ b) * 2 + c) for j in range(ny) for c, b in enumerate((bit0, bit1))]
        return lax.ppermute(v, axes, pairs)

    def swap(v):
        return lax.ppermute(v, "dp", [(0, 1), (1, 0)])

    def layer(x, wg, wu, wd, dy):
        i = lax.axis_index("dp").astype(jnp.int32).reshape(1)
        ka = 1792
        qa = 304
        sizes = (448, 256, 48, 16)
        x1, x2 = hop(x, 1, 2), hop(x, 2, 1)
        xX, xY = jnp.where(i[0] == 0, x1, x2), jnp.where(i[0] == 0, x2, x1)
        dyX, dyY = hop(dy, 1, 1), hop(dy, 2, 2)
        wgo, wuo, wdo = swap(wg), swap(wu), swap(wd)
        wXa, wXb = hop(wd[:ka], 1, 1), hop(wd[ka:], 1, 1)
        xD = hop(xX, 2, 2)
        qb = qa + 8
        hd = wg.shape[0]
        part = jnp.where(i[0] == 0, dyY[:qb], dyX[:qb])
        dyDa = hop(part[:qa], 1, 2)
        dyDc = hop(part[qa:, :hd], 1, 2)
        dyDe = hop(dyX[qa:qb, hd:], 2, 2)
        dyDb = hop(dyX[qb:], 2, 2)
        dyD = jnp.concatenate([dyDa, jnp.concatenate([dyDc, dyDe], axis=1), dyDb], axis=0)
        wX = (wXa, wXb, swap(wXa), swap(wXb))

        a0, b0, h0, hall, xall, wgc, wuc = k_fwd0(i, x, wg, wgo, wu, wuo)
        *alls, wdc = k_g0(i, dy, wd, wdo, a0, b0)
        a1, b1, h1, hall, xall = k_fwd(i, 1, xX, wgc, wuc, hall, xall)
        a2, b2, h2, hall, xall = k_fwd(i, 2, xY, wgc, wuc, hall, xall)
        a3, b3, h3, hall, xall = k_fwd(i, 3, xD, wgc, wuc, hall, xall)

        alls = k_g(i, 1, dyX, wdc, a1, b1, alls)
        alls = k_g(i, 2, dyY, wdc, a2, b2, alls)
        z1 = k_dx(i, lambda c: 1 + c, alls[0], alls[1], wgc, wuc)
        s1 = hop(z1, 1, 2)
        z0 = k_dx(i, lambda c: 0, alls[0], alls[1], wgc, wuc, add=dy)
        daall, dball, dyall = k_g(i, 3, dyD, wdc, a3, b3, alls, (z0, z1))
        z3 = k_dx(i, lambda c: 3, daall, dball, wgc, wuc)
        sa = hop(z3, 1, 2)
        z2 = k_dx(i, lambda c: 2 - c, daall, dball, wgc, wuc)
        s2 = k_add(i, z2, sa, sizes)
        s2 = [hop(v, 2, 1) for v in s2]

        hDr, hXr = hop(h3, 1, 1), hop(h1, 1, 1)
        yYr = hop(k_y2(i, h2, wdc, hDr, wX), 2, 2)
        y = k_y2(i, h0, wdc, hXr, wX, (x, yYr))

        xallo, hallo = swap(xall), swap(hall)
        dyallo, daallo, dballo = swap(dyall), swap(daall), swap(dball)
        dwd = k_dwd(i, hall, hallo, dyall, dyallo)
        dwg = k_dw(i, xall, xallo, daall, daallo)
        dwu = k_dw(i, xall, xallo, dball, dballo)

        pre = k_add(i, z0, s1)[0]
        dx = ()
        for p, v in enumerate(s2[:3]):
            dx = (k_fin(i, sum(sizes[:p]), pre, v, dx, 64 if p < 2 else 16),)
        dx = lax.dynamic_update_slice(dx[0], (pre[752:] + s2[3]).astype(bf), (752, 0))
        return y, dx, dwg, dwu, dwd

    return jax.shard_map(layer, mesh=mesh, in_specs=(rows, wsp, wsp, dsp, rows), out_specs=(rows, rows, wsp, wsp, dsp), check_vma=False)
```
